512 devices in a mesh: section: 64 (over z_lo, y, core), dp: 8 (over x, z_hi).
Axes of the slice: x: 4, y: 8, z: 8 (z_hi: 2, z_lo: 4; z = z_hi * 4 + z_lo), core: 2. Of those that a mesh axis runs over, the one named last changes fastest.
Arguments:
- layer_in: bfloat16 [64, 1024, 5120], P('section', 'dp'), may hold values from -6 to 6
- latent: bfloat16 [64, 1024, 384], P('section', 'dp'), may hold values from -6 to 6
- mix_grad: bfloat16 [64, 1024, 5120], P('section', 'dp'), may hold values from -0.1875 to 0.1875
- down_proj: bfloat16 [64, 5120, 384], P('section', 'dp'), may hold values from -0.078125 to 0.078125
- up_proj: bfloat16 [64, 384, 5120], P('section', None, 'dp'), may hold values from -0.3125 to 0.3125
- norm_gain: bfloat16 [64, 5120], P('section', 'dp'), may hold values from 0.5 to 1.5
- mix_weight: float32 [64, 8], P('section'), may hold values from 0.2 to 1
Outputs:
- up_grad: bfloat16 [64, 384, 5120], P('section', None, 'dp')
- down_grad: bfloat16 [64, 5120, 384], P('section', 'dp')
- gain_grad: float32 [64, 5120], P('section', 'dp')
- mixing_grad: float32 [64, 8], P('section')
The draws below stay inside these ranges and needn't reach their ends.
All inputs are finite; a program needn't handle non-finite values.
Results may differ from the reference program's by a relative error of at most 0.0064.
Values may be sent and summed in bfloat16 or wider, within the bound.
No kernel may reach another device: no remote copies, remote signals or barrier semaphores. Data moves between devices by JAX's collectives and lax.ppermute only.
A program may use at most 128 MiB of HBM per device.

```python
import jax
import jax.numpy as jnp
from jax import lax

D = 5120
R = 384
MIXES = 8
LAYERS = 64
TOKENS = 1024


def steps_of(stream_key, dims, cuts, least, largest):
    def one(axis_at, blocks):
        steps = jax.random.uniform(jax.random.fold_in(jax.random.fold_in(stream_key, 6), axis_at), (blocks,), jnp.float32, least / len(cuts), largest / len(cuts))
        return jnp.repeat(jnp.exp(steps), dims[axis_at] // blocks).reshape((-1,) + (1,) * (len(dims) - axis_at - 1))

    level = one(*cuts[0])
    for cut in cuts[1:]:
        level = level * one(*cut)
    return level


def gaussian(stream_key, extent, scale, bound, split=(), held_as=jnp.bfloat16):
    loudness = steps_of(stream_key, extent, split, -0.22, 0.18) if split else 1.0
    array = jax.random.normal(stream_key, extent, jnp.float32) * scale * loudness
    return jnp.minimum(jnp.maximum(array, -bound), bound).astype(held_as)


def setup_inputs(seed: int = 0) -> dict:
    arg_keys = jax.random.split(jax.random.key(seed), 8)
    layer_in = gaussian(arg_keys[0], (LAYERS, TOKENS, D), 1.0, 6.0, ((0, 64), (1, 8)))
    latent = gaussian(arg_keys[1], (LAYERS, TOKENS, R), 1.0, 6.0, ((0, 64), (1, 8)))
    mix_grad = gaussian(arg_keys[2], (LAYERS, TOKENS, D), (TOKENS ** -0.5), 0.1875, ((0, 64), (1, 8)))
    down_proj = gaussian(arg_keys[3], (LAYERS, D, R), D ** -0.5, 0.078125, ((0, 64), (1, 8)))
    up_proj = gaussian(arg_keys[4], (LAYERS, R, D), R ** -0.5, 0.3125, ((0, 64), (2, 8)))
    norm_gain = jnp.clip(1.0 + 0.1 * jax.random.normal(arg_keys[5], (LAYERS, D), jnp.float32), 0.5, 1.5).astype(jnp.bfloat16)
    mix_weight = jnp.clip(0.2 + 0.8 * jax.random.uniform(arg_keys[6], (LAYERS, MIXES), jnp.float32) ** steps_of(arg_keys[6], (LAYERS, MIXES), ((0, 64),), -0.2, 0.2), 0.2, 1.0)
    return {"layer_in": layer_in, "latent": latent, "mix_grad": mix_grad, "down_proj": down_proj, "up_proj": up_proj, "norm_gain": norm_gain, "mix_weight": mix_weight}


epsilon = 1e-06
root_coef = 0.7978845608028654

def gelu_pair(values):
    tangent = jnp.tanh(root_coef * (values + 0.044715 * values * values * values))
    result = 0.5 * values * (1.0 + tangent)
    slopes = 0.5 * (1.0 + tangent) + 0.5 * values * (1.0 - tangent * tangent) * root_coef * (1.0 + 3.0 * 0.044715 * values * values)
    return (result, slopes)

def reference(layer_in, latent, mix_grad, down_proj, up_proj, norm_gain, mix_weight):
    stride = LAYERS // MIXES

    def one_section(index):
        inputs = lax.dynamic_index_in_dim(layer_in, index, 0, False).astype(jnp.float32)
        mean_sq = lax.optimization_barrier(jnp.mean(inputs * inputs, axis=1, keepdims=True))
        inv_rms = lax.rsqrt(mean_sq + epsilon)
        scaled = inputs * inv_rms
        gain_row = lax.dynamic_index_in_dim(norm_gain, index, 0, False).astype(jnp.float32)
        normed = (scaled * gain_row).astype(jnp.bfloat16)
        latent_row = lax.dynamic_index_in_dim(latent, index, 0, False).astype(jnp.float32)
        activated, slopes = gelu_pair(latent_row)
        act_half = activated.astype(jnp.bfloat16)
        up_block = lax.dynamic_index_in_dim(up_proj, index, 0, False)
        down_block = lax.dynamic_index_in_dim(down_proj, index, 0, False)
        layer_out = inputs + jnp.dot(act_half, up_block, preferred_element_type=jnp.float32)
        weight_row = lax.dynamic_index_in_dim(mix_weight, index, 0, False)
        grad_sum = jnp.zeros(inputs.shape, jnp.float32)
        products = []
        for member in range(MIXES):
            target = index + member * stride
            inside = (target < LAYERS).astype(jnp.float32)
            clamped = jnp.minimum(target, LAYERS - 1).astype(jnp.int32)
            piece = lax.dynamic_index_in_dim(mix_grad, clamped, 0, False).astype(jnp.float32) * inside
            products.append(jnp.sum(piece * layer_out))
            grad_sum = grad_sum + weight_row[member] * piece
        grad_half = grad_sum.astype(jnp.bfloat16)
        act_grad = jnp.dot(grad_half, up_block.T, preferred_element_type=jnp.float32)
        latent_grad = (act_grad * slopes).astype(jnp.bfloat16)
        up_grad = jnp.dot(act_half.T, grad_half, preferred_element_type=jnp.float32).astype(jnp.bfloat16)
        down_grad = jnp.dot(normed.T, latent_grad, preferred_element_type=jnp.float32).astype(jnp.bfloat16)
        norm_grad = jnp.dot(latent_grad, down_block.T, preferred_element_type=jnp.float32)
        gain_grad = lax.optimization_barrier(jnp.sum(norm_grad * scaled, axis=0))
        return (up_grad, down_grad, gain_grad, jnp.stack(products))
    up_grad, down_grad, gain_grad, mixing_grad = lax.map(one_section, jnp.arange(LAYERS, dtype=jnp.int32))
    return (up_grad, down_grad, gain_grad, mixing_grad)
```

```python
import jax
import jax.numpy as jnp
from jax import lax
from jax.experimental import pallas as pl
from jax.experimental.pallas import tpu as pltpu
from jax.sharding import Mesh, PartitionSpec as P

MIXES = 8
epsilon = 1e-06
root_coef = 0.7978845608028654
GROUP = ("zl", "yh")


def gelu_pair(values):
    tangent = jnp.tanh(root_coef * (values + 0.044715 * values * values * values))
    result = 0.5 * values * (1.0 + tangent)
    slopes = 0.5 * (1.0 + tangent) + 0.5 * values * (1.0 - tangent * tangent) * root_coef * (
        1.0 + 3.0 * 0.044715 * values * values
    )
    return (result, slopes)


def exchange(pieces, axes):
    return lax.all_to_all(pieces, axes, split_axis=0, concat_axis=0, tiled=True)


def swapped(value, axis):
    return lax.ppermute(value, axis, [(0, 1), (1, 0)])


def shifted(value, axis, steps):
    count = lax.axis_size(axis)
    return lax.ppermute(value, axis, [(i, (i + steps) % count) for i in range(count)])


def mix_body(coef, grads, out):
    halves, sections, rows, cols = grads.shape
    for half in range(halves):
        for at in range(0, cols, 128):
            lanes = slice(at, at + 128)
            tiles = [grads[half, k, :, lanes].astype(jnp.float32) for k in range(sections)]
            for k in range(sections):
                total = coef[k, 0] * tiles[k]
                for m in range(1, sections - k):
                    total = total + coef[k, m] * tiles[k + m]
                out[k, half, :, lanes] = total.astype(jnp.bfloat16)


def mix(weights, grads):
    halves, sections, rows, cols = grads.shape
    block = 640
    return pl.pallas_call(
        mix_body,
        grid=(cols // block,),
        in_specs=[
            pl.BlockSpec(memory_space=pltpu.SMEM),
            pl.BlockSpec((halves, sections, rows, block), lambda j: (0, 0, 0, j)),
        ],
        out_specs=pl.BlockSpec((sections, halves, rows, block), lambda j: (0, 0, 0, j)),
        out_shape=jax.ShapeDtypeStruct((sections, halves, rows, cols), jnp.bfloat16),
        name="mix",
    )(weights, grads)


def gram_body(grads, outs, result):
    halves, sections, rows, cols = grads.shape
    sums = {}
    for half in range(halves):
        for at in range(0, cols, 128):
            lanes = slice(at, at + 128)
            left = [outs[k, half, :, lanes].astype(jnp.float32) for k in range(sections)]
            right = [grads[half, k, :, lanes].astype(jnp.float32) for k in range(sections)]
            for k in range(sections):
                for m in range(sections - k):
                    product = left[k] * right[k + m]
                    folded = product[:8] + product[8:]
                    sums[k, m] = folded if (k, m) not in sums else sums[k, m] + folded

    @pl.when(pl.program_id(0) == 0)
    def _():
        result[...] = jnp.zeros(result.shape, jnp.float32)

    for (k, m), total in sums.items():
        result[k * MIXES + m] += total


def gram(grads, outs):
    halves, sections, rows, cols = grads.shape
    block = 640
    return pl.pallas_call(
        gram_body,
        grid=(cols // block,),
        in_specs=[
            pl.BlockSpec((halves, sections, rows, block), lambda j: (0, 0, 0, j)),
            pl.BlockSpec((sections, halves, rows, block), lambda j: (0, 0, 0, j)),
        ],
        out_specs=pl.BlockSpec((sections * MIXES, 8, 128), lambda j: (0, 0, 0)),
        out_shape=jax.ShapeDtypeStruct((sections * MIXES, 8, 128), jnp.float32),
        name="gram",
    )(grads, outs)


def local(layer_in, latent, mix_grad, down_proj, up_proj, norm_gain, mix_weight):
    layer_in, latent, mix_grad = (layer_in[0], latent[0], mix_grad[0])
    tokens, width = layer_in.shape
    xs, zs = (lax.axis_size("x"), lax.axis_size("zh"))
    sections = lax.axis_size("zl") * lax.axis_size("yh")
    block = width // (xs * zs)
    rows = tokens // sections
    at_x, at_zh, at_zl, at_yh = [lax.axis_index(a) for a in ("x", "zh", "zl", "yh")]
    first = at_zh == 0

    def feature_half(array, half):
        return jnp.concatenate(
            [array[:, (i * zs + half) * block : (i * zs + half + 1) * block] for i in range(xs)], axis=1
        )

    def both_halves(own, other):
        own, other = [t.reshape(sections, rows, *t.shape[1:]) for t in (own, other)]
        pair = jnp.stack([jnp.where(first, own, other), jnp.where(first, other, own)], axis=1)
        return pair.reshape(2 * tokens, *own.shape[2:])

    grads = jnp.stack([feature_half(mix_grad, 0), feature_half(mix_grad, 1)])
    grads = exchange(grads.reshape(zs * sections, rows, xs * block), ("zh", *GROUP))
    grads = grads.reshape(zs, sections, rows, xs * block)

    own_weight = mix_weight[0]
    other_weight = swapped(own_weight, "yh")
    pair = jnp.stack(
        [jnp.where(at_yh == 0, own_weight, other_weight), jnp.where(at_yh == 0, other_weight, own_weight)]
    )
    places = lax.axis_size("zl")
    weights = jnp.zeros((places, *pair.shape), jnp.float32)
    for step in range(places):
        piece = shifted(pair, "zl", step) if step else pair
        here = (jnp.arange(places) == (at_zl - step) % places)[:, None, None]
        weights = jnp.where(here, piece[None], weights)
    weights = weights.reshape(sections, MIXES)

    half_0, half_1 = (feature_half(layer_in, 0), feature_half(layer_in, 1))
    kept = jnp.where(first, half_0, half_1)
    inputs = both_halves(kept, swapped(jnp.where(first, half_1, half_0), "zh"))
    wide = layer_in.astype(jnp.float32)
    own_rms = lax.rsqrt(jnp.sum(wide * wide, axis=1) / width + epsilon)
    inv_rms = both_halves(own_rms, swapped(own_rms, "zh"))
    latents = both_halves(latent, swapped(latent, "zh"))
    activated, slopes = gelu_pair(latents.astype(jnp.float32))
    act_half = activated.astype(jnp.bfloat16)

    up_block = up_proj[0]
    parts = jnp.stack([up_block] + [shifted(up_block, "x", step) for step in range(1, xs)])
    up_half = jnp.concatenate(
        [lax.dynamic_index_in_dim(parts, (at_x - i) % xs, 0, False) for i in range(xs)], axis=1
    )

    branch = jnp.dot(act_half, up_half, preferred_element_type=jnp.float32)
    layer_out = (inputs.astype(jnp.float32) + branch).astype(jnp.bfloat16)

    mixed = mix(weights, grads)
    out_grad = exchange(mixed, GROUP).reshape(2 * tokens, xs * block)

    outs = exchange(layer_out.reshape(sections, zs, rows, xs * block), GROUP)
    products = jnp.sum(gram(grads, outs), axis=(1, 2)).reshape(sections, MIXES)
    spread = jnp.broadcast_to(products[:, None], (sections, xs * zs, MIXES))
    mixing = exchange(spread.reshape(sections * xs * zs, MIXES), (*GROUP, "x", "zh")).sum(axis=0)

    act_partial = jnp.einsum("tc,rc->tr", out_grad, up_half, preferred_element_type=jnp.float32)
    act_other = swapped(act_partial.astype(jnp.bfloat16), "zh").astype(jnp.float32)
    scaled_grad = ((act_partial + act_other) * slopes * inv_rms[:, None]).astype(jnp.bfloat16)

    def by_x(array):
        return jnp.stack([array[:, i * block : (i + 1) * block] for i in range(xs)])

    def to_all_x(array):
        return exchange(jnp.broadcast_to(array, (xs, *array.shape)), "x")

    all_inputs = exchange(by_x(inputs), "x")
    all_grads = exchange(by_x(out_grad), "x")
    all_act = to_all_x(act_half)
    all_latent_grads = to_all_x(scaled_grad)

    up_grad = jnp.einsum(
        "xtr,xtc->rc", all_act, all_grads, preferred_element_type=jnp.float32
    ).astype(jnp.bfloat16)
    gram_grad = jnp.einsum(
        "xtc,xtr->cr", all_inputs, all_latent_grads, preferred_element_type=jnp.float32
    )
    gain = norm_gain[0].astype(jnp.float32)
    down_grad = (gram_grad * gain[:, None]).astype(jnp.bfloat16)
    gain_grad = jnp.sum(gram_grad * down_proj[0].astype(jnp.float32), axis=1)
    return (up_grad[None], down_grad[None], gain_grad[None], mixing[None])


def solution(mesh):
    devices = mesh.devices.reshape(4, 2, 8, 4, 2)
    fine = Mesh(devices, ("zl", "yh", "r", "x", "zh"))
    section, dp = (("zl", "yh", "r"), ("x", "zh"))
    return jax.shard_map(
        local,
        mesh=fine,
        in_specs=(
            P(section, dp, None),
            P(section, dp, None),
            P(section, dp, None),
            P(section, dp, None),
            P(section, None, dp),
            P(section, dp),
            P(section, None),
        ),
        out_specs=(
            P(section, None, dp),
            P(section, dp, None),
            P(section, dp),
            P(section, None),
        ),
        check_vma=False,
    )
```

```python
import jax
import jax.numpy as jnp
from jax import lax
from jax.experimental import pallas as pl
from jax.experimental.pallas import tpu as pltpu
from jax.sharding import Mesh, PartitionSpec as P

MIXES = 8
LANES = 128
BLOCK = 640
TERMS = 3
epsilon = 1e-06
root_coef = 0.7978845608028654
GROUP = ("zl", "yh")
SMEM = pl.BlockSpec(memory_space=pltpu.SMEM)


def gelu_pair(values):
    tangent = jnp.tanh(root_coef * (values + 0.044715 * values * values * values))
    result = 0.5 * values * (1.0 + tangent)
    slopes = 0.5 * (1.0 + tangent) + 0.5 * values * (1.0 - tangent * tangent) * root_coef * (
        1.0 + 3.0 * 0.044715 * values * values
    )
    return (result, slopes)


def exchange(pieces, axes):
    return lax.all_to_all(pieces, axes, split_axis=0, concat_axis=0, tiled=True)


def swapped(value, axis):
    return lax.ppermute(value, axis, [(0, 1), (1, 0)])


def shifted(value, axis, steps):
    count = lax.axis_size(axis)
    return lax.ppermute(value, axis, [(i, (i + steps) % count) for i in range(count)])


def split_terms(value):
    terms = []
    for _ in range(TERMS):
        term = value.astype(jnp.bfloat16).astype(jnp.float32)
        terms.append(term)
        value = value - term
    return terms


def shape(dims, dtype=jnp.bfloat16):
    return jax.ShapeDtypeStruct(dims, dtype)


def pack_grads_body(weights, grads, out):
    halves, sections, rows, cols = out.shape
    block = BLOCK
    for half in range(halves):
        for i in range((cols - LANES) // block):
            piece = grads[:, (i * halves + half) * block : (i * halves + half + 1) * block]
            out[half, :, :, i * block : (i + 1) * block] = piece.reshape(sections, rows, block)
    lane = lax.broadcasted_iota(jnp.int32, (rows, LANES), 1)
    row = lax.broadcasted_iota(jnp.int32, (rows, LANES), 0)
    value = jnp.zeros((rows, LANES), jnp.float32)
    for m in range(MIXES):
        value = jnp.where(lane == m, weights[0, m], value)
    tail = jnp.zeros((rows, LANES), jnp.float32)
    for i, term in enumerate(split_terms(value)):
        tail = jnp.where(row == i, term, tail)
    tail = tail.astype(jnp.bfloat16)
    for half in range(halves):
        for k in range(sections):
            out[half, k, :, cols - LANES :] = tail


def pack_inputs_body(place, layer_in, latent, kept, sent):
    tokens, cols = kept.shape
    ranks = latent.shape[1]
    half_cols = cols - ranks - LANES
    width = layer_in.shape[1]
    block = BLOCK
    first = place[0] == 0
    squares = jnp.zeros((tokens, LANES), jnp.float32)
    for at in range(0, width, LANES):
        tile = layer_in[:, at : at + LANES].astype(jnp.float32)
        squares = squares + tile * tile
    inv_rms = lax.rsqrt(jnp.sum(squares, axis=1, keepdims=True) / width + epsilon)
    lane = lax.broadcasted_iota(jnp.int32, (tokens, LANES), 1)
    tail = jnp.zeros((tokens, LANES), jnp.float32)
    for i, term in enumerate(split_terms(jnp.broadcast_to(inv_rms, (tokens, LANES)))):
        tail = jnp.where(lane == i, term, tail)
    tail = tail.astype(jnp.bfloat16)
    for i in range(half_cols // block):
        low = layer_in[:, 2 * i * block : (2 * i + 1) * block]
        high = layer_in[:, (2 * i + 1) * block : (2 * i + 2) * block]
        kept[:, i * block : (i + 1) * block] = jnp.where(first, low, high)
        sent[:, i * block : (i + 1) * block] = jnp.where(first, high, low)
    for out in (kept, sent):
        out[:, half_cols : half_cols + ranks] = latent[...]
        out[:, half_cols + ranks :] = tail


def lift_body(place, kept, other, kept_rest, other_rest, up_0, up_1, up_2, up_3, sends, moves, up_half, scale, act):
    sections, _, halves, rows, block = sends.shape
    ranks = up_0.shape[0]
    at = pl.program_id(0)
    first = place[0] == 0

    def in_order(own, far, half):
        return jnp.where(first, own, far) if half == 0 else jnp.where(first, far, own)

    @pl.when(at == 0)
    def _():
        for half in range(halves):
            rest = in_order(kept_rest[...], other_rest[...], half).astype(jnp.float32)
            values, slopes = gelu_pair(rest[:, :, :ranks])
            inv_rms = jnp.sum(rest[:, :, ranks : ranks + LANES], axis=2, keepdims=True)
            act[:, half] = values.astype(jnp.bfloat16)
            scale[:, half] = slopes * inv_rms

    turn = lax.rem(place[1] - at + 4, 4)
    up = jnp.where(turn == 0, up_0[...], jnp.where(turn == 1, up_1[...], jnp.where(turn == 2, up_2[...], up_3[...])))
    up_half[...] = up
    for half in range(halves):
        rows_in = in_order(kept[...], other[...], half)
        moves[0, :, half, :, :block] = rows_in
        moves[0, :, half, :, block:] = act[:, half]
        branch = jnp.dot(
            act[:, half].reshape(sections * rows, ranks), up, preferred_element_type=jnp.float32
        ).reshape(sections, rows, block)
        sends[:, 0, half] = (rows_in.astype(jnp.float32) + branch).astype(jnp.bfloat16)


def mix_body(coef, grads, sends, out):
    halves, sections, rows, cols = grads.shape
    for half in range(halves):
        for at in range(0, cols, LANES):
            lanes = slice(at, at + LANES)
            tiles = [grads[half, k, :, lanes].astype(jnp.float32) for k in range(sections)]
            for k in range(sections):
                total = coef[k, 0] * tiles[k]
                for m in range(1, sections - k):
                    total = total + coef[k, m] * tiles[k + m]
                out[k, 0, half, :, lanes] = total.astype(jnp.bfloat16)


def gram_body(grads, outs, result):
    halves, sections, rows, cols = grads.shape
    sums = {}
    for half in range(halves):
        for at in range(0, cols, LANES):
            lanes = slice(at, at + LANES)
            left = [outs[k, 0, half, :, lanes].astype(jnp.float32) for k in range(sections)]
            right = [grads[half, k, :, lanes].astype(jnp.float32) for k in range(sections)]
            for k in range(sections):
                for m in range(sections - k):
                    product = left[k] * right[k + m]
                    folded = product[:8] + product[8:]
                    sums[k, m] = folded if (k, m) not in sums else sums[k, m] + folded

    @pl.when(pl.program_id(0) == 0)
    def _():
        result[...] = jnp.zeros(result.shape, jnp.float32)

    for (k, m), total in sums.items():
        result[k * MIXES + m] += total


def act_grad_body(grads, up, moves, total, rounded):
    sections, _, halves, rows, block = grads.shape
    at = pl.program_id(0)
    piece = grads[...].reshape(sections * halves * rows, block)
    moves[0] = piece
    part = lax.dot_general(piece, up[...], (((1,), (1,)), ((), ())), preferred_element_type=jnp.float32)

    @pl.when(at == 0)
    def _():
        total[...] = part

    @pl.when(at != 0)
    def _():
        total[...] += part

    @pl.when(at == pl.num_programs(0) - 1)
    def _():
        rounded[...] = total[...].astype(jnp.bfloat16)


def up_grad_body(place, grads, act_0, act_1, act_2, act_3, out):
    total = jnp.zeros(out.shape, jnp.float32)
    for step, act in enumerate((act_0, act_1, act_2, act_3)):
        source = lax.rem(place[1] - step + 4, 4)
        total = total + lax.dot_general(
            act[:, grads.shape[2] :], grads[source], (((0,), (0,)), ((), ())), preferred_element_type=jnp.float32
        )
    out[...] = total.astype(jnp.bfloat16)


def down_grad_body(in_0, in_1, in_2, in_3, lat_0, lat_1, lat_2, lat_3, gain, down, out, gain_out):
    total = jnp.zeros(out.shape, jnp.float32)
    for inputs, latents in ((in_0, lat_0), (in_1, lat_1), (in_2, lat_2), (in_3, lat_3)):
        total = total + lax.dot_general(
            inputs[...], latents[...], (((0,), (0,)), ((), ())), preferred_element_type=jnp.float32
        )
    gain_cols = jnp.transpose(jnp.broadcast_to(gain[...].astype(jnp.float32), (8, gain.shape[1])))
    out[...] = (total * gain_cols[:, :1]).astype(jnp.bfloat16)
    product = total * down[...].astype(jnp.float32)
    ones = jnp.ones((8, product.shape[1]), jnp.float32)
    sums = lax.dot_general(
        ones, product, (((1,), (1,)), ((), ())), precision=lax.Precision.HIGHEST, preferred_element_type=jnp.float32
    )
    gain_out[...] = sums[:1]


def local(layer_in, latent, mix_grad, down_proj, up_proj, norm_gain, mix_weight):
    layer_in, latent, mix_grad = (layer_in[0], latent[0], mix_grad[0])
    tokens, width = layer_in.shape
    ranks = latent.shape[1]
    xs, zs = (lax.axis_size("x"), lax.axis_size("zh"))
    sections = lax.axis_size("zl") * lax.axis_size("yh")
    block = width // (xs * zs)
    half_width = xs * block
    rows = tokens // sections
    place = jnp.stack([lax.axis_index("zh"), lax.axis_index("x")]).astype(jnp.int32)

    packed = pl.pallas_call(
        pack_grads_body,
        in_specs=[SMEM, pl.BlockSpec((tokens, width), lambda: (0, 0))],
        out_specs=pl.BlockSpec((zs, sections, rows, half_width + LANES), lambda: (0, 0, 0, 0)),
        out_shape=shape((zs, sections, rows, half_width + LANES)),
        name="pack_grads",
    )(mix_weight, mix_grad)
    grads = exchange(packed.reshape(zs * sections, rows, half_width + LANES), ("zh", *GROUP))
    grads = grads.reshape(zs, sections, rows, half_width + LANES)

    full = half_width + ranks + LANES
    kept, sent = pl.pallas_call(
        pack_inputs_body,
        in_specs=[SMEM, pl.BlockSpec((tokens, width), lambda: (0, 0)), pl.BlockSpec((tokens, ranks), lambda: (0, 0))],
        out_specs=[pl.BlockSpec((tokens, full), lambda: (0, 0))] * 2,
        out_shape=[shape((tokens, full))] * 2,
        name="pack_inputs",
    )(place, layer_in, latent)
    other = swapped(sent, "zh")

    up_block = up_proj[0]
    ups = [up_block] + [shifted(up_block, "x", step) for step in range(1, xs)]

    kept, other = [t.reshape(sections, rows, full) for t in (kept, other)]
    wide = pl.BlockSpec((sections, rows, block), lambda a: (0, 0, a))
    rest = ranks + LANES
    narrow = pl.BlockSpec((sections, rows, rest), lambda a: (0, 0, half_width // rest))
    whole_up = pl.BlockSpec((ranks, block), lambda a: (0, 0))
    sends, moves, up_half, scale = pl.pallas_call(
        lift_body,
        grid=(xs,),
        in_specs=[SMEM, wide, wide, narrow, narrow] + [whole_up] * xs,
        out_specs=[
            pl.BlockSpec((sections, 1, zs, rows, block), lambda a: (0, 1, 0, 0, a)),
            pl.BlockSpec((1, sections, zs, rows, block + ranks), lambda a: (a, 0, 0, 0, 0)),
            pl.BlockSpec((ranks, block), lambda a: (0, a)),
            pl.BlockSpec((sections, zs, rows, ranks), lambda a: (0, 0, 0, 0)),
        ],
        out_shape=[
            shape((sections, 2, zs, rows, half_width)),
            shape((xs, sections, zs, rows, block + ranks)),
            shape((ranks, half_width)),
            shape((sections, zs, rows, ranks), jnp.float32),
        ],
        scratch_shapes=[pltpu.VMEM((sections, zs, rows, ranks), jnp.bfloat16)],
        name="lift",
    )(place, kept, other, kept, other, *ups)
    scale = scale.reshape(zs * tokens, ranks)

    weights = jnp.sum(grads[0, :, :TERMS, half_width : half_width + MIXES].astype(jnp.float32), axis=1)
    grads_spec = pl.BlockSpec((zs, sections, rows, block), lambda a: (0, 0, 0, a))
    sends = pl.pallas_call(
        mix_body,
        grid=(xs,),
        in_specs=[SMEM, grads_spec, pl.BlockSpec(memory_space=pl.ANY)],
        out_specs=pl.BlockSpec((sections, 1, zs, rows, block), lambda a: (0, 0, 0, 0, a)),
        out_shape=shape(sends.shape),
        input_output_aliases={2: 0},
        name="mix",
    )(weights, grads, sends)
    arrived = exchange(sends, GROUP)

    moves = moves.reshape(xs, zs * tokens, block + ranks)
    at_x = place[1]
    moved = [lax.dynamic_index_in_dim(moves, at_x, 0, False)]
    for step in range(1, xs):
        moved.append(shifted(lax.dynamic_index_in_dim(moves, (at_x + step) % xs, 0, False), "x", step))

    arrived, *moved = lax.optimization_barrier((arrived, *moved))
    by_x, act_partial, act_rounded = pl.pallas_call(
        act_grad_body,
        grid=(xs,),
        in_specs=[
            pl.BlockSpec((sections, 1, zs, rows, block), lambda a: (0, 0, 0, 0, a)),
            pl.BlockSpec((ranks, block), lambda a: (0, a)),
        ],
        out_specs=[
            pl.BlockSpec((1, zs * tokens, block), lambda a: (a, 0, 0)),
            pl.BlockSpec((zs * tokens, ranks), lambda a: (0, 0)),
            pl.BlockSpec((zs * tokens, ranks), lambda a: (0, 0)),
        ],
        out_shape=[
            shape((xs, zs * tokens, block)),
            shape((zs * tokens, ranks), jnp.float32),
            shape((zs * tokens, ranks)),
        ],
        name="act_grad",
    )(arrived, up_half)
    act_other = swapped(act_rounded, "zh").astype(jnp.float32)
    all_grads = exchange(by_x, "x")
    scaled_grad = ((act_partial + act_other) * scale).astype(jnp.bfloat16)
    latent_grads = [scaled_grad] + [shifted(scaled_grad, "x", step) for step in range(1, xs)]

    gram_grads, _ = lax.optimization_barrier((grads, act_rounded))
    products = pl.pallas_call(
        gram_body,
        grid=(xs,),
        in_specs=[grads_spec, pl.BlockSpec((sections, 1, zs, rows, block), lambda a: (0, 1, 0, 0, a))],
        out_specs=pl.BlockSpec((sections * MIXES, 8, LANES), lambda a: (0, 0, 0)),
        out_shape=shape((sections * MIXES, 8, LANES), jnp.float32),
        name="gram",
    )(gram_grads, arrived)
    products = jnp.sum(products, axis=(1, 2)).reshape(sections, MIXES)
    spread = jnp.broadcast_to(products[:, None], (sections, xs * zs, MIXES))
    spread, all_grads = lax.optimization_barrier((spread, all_grads))
    mixing = exchange(spread.reshape(sections * xs * zs, MIXES), (*GROUP, "x", "zh")).sum(axis=0)

    up_grad = pl.pallas_call(
        up_grad_body,
        in_specs=[SMEM, pl.BlockSpec((xs, zs * tokens, block), lambda: (0, 0, 0))]
        + [pl.BlockSpec((zs * tokens, block + ranks), lambda: (0, 0))] * xs,
        out_specs=pl.BlockSpec((ranks, block), lambda: (0, 0)),
        out_shape=shape((ranks, block)),
        name="up_grad",
    )(place, all_grads, *moved)

    down_grad, gain_grad = pl.pallas_call(
        down_grad_body,
        grid=(1,),
        in_specs=[pl.BlockSpec((zs * tokens, block), lambda a: (0, 0))] * xs
        + [pl.BlockSpec((zs * tokens, ranks), lambda a: (0, 0))] * xs
        + [pl.BlockSpec((1, block), lambda a: (0, 0)), pl.BlockSpec((block, ranks), lambda a: (0, 0))],
        out_specs=[pl.BlockSpec((block, ranks), lambda a: (0, 0)), pl.BlockSpec((1, block), lambda a: (0, 0))],
        out_shape=[shape((block, ranks)), shape((1, block), jnp.float32)],
        name="down_grad",
    )(*moved, *latent_grads, norm_gain, down_proj[0])
    return (up_grad[None], down_grad[None], gain_grad, mixing[None])


def solution(mesh):
    devices = mesh.devices.reshape(4, 2, 8, 4, 2)
    fine = Mesh(devices, ("zl", "yh", "r", "x", "zh"))
    section, dp = (("zl", "yh", "r"), ("x", "zh"))
    return jax.shard_map(
        local,
        mesh=fine,
        in_specs=(
            P(section, dp, None),
            P(section, dp, None),
            P(section, dp, None),
            P(section, dp, None),
            P(section, None, dp),
            P(section, dp),
            P(section, None),
        ),
        out_specs=(
            P(section, None, dp),
            P(section, dp, None),
            P(section, dp),
            P(section, None),
        ),
        check_vma=False,
    )
```

```python
import jax
import jax.numpy as jnp
from jax import lax
from jax.experimental import pallas as pl
from jax.experimental.pallas import tpu as pltpu
from jax.sharding import Mesh, PartitionSpec as P


MIXES = 8
LANES = 128
BLOCK = 640
TERMS = 3
epsilon = 1e-06
root_coef = 0.7978845608028654
GROUP = ("zl", "yh")
SMEM = pl.BlockSpec(memory_space=pltpu.SMEM)


def gelu_pair(values):
    tangent = jnp.tanh(root_coef * (values + 0.044715 * values * values * values))
    result = 0.5 * values * (1.0 + tangent)
    slopes = 0.5 * (1.0 + tangent) + 0.5 * values * (1.0 - tangent * tangent) * root_coef * (
        1.0 + 3.0 * 0.044715 * values * values
    )
    return (result, slopes)


def exchange(pieces, axes):
    return lax.all_to_all(pieces, axes, split_axis=0, concat_axis=0, tiled=True)


def swapped(value, axis):
    return lax.ppermute(value, axis, [(0, 1), (1, 0)])


def shifted(value, axis, steps):
    count = lax.axis_size(axis)
    return lax.ppermute(value, axis, [(i, (i + steps) % count) for i in range(count)])


def split_terms(value):
    terms = []
    for _ in range(TERMS):
        term = value.astype(jnp.bfloat16).astype(jnp.float32)
        terms.append(term)
        value = value - term
    return terms


def shape(dims, dtype=jnp.bfloat16):
    return jax.ShapeDtypeStruct(dims, dtype)


def pack_grads_body(weights, grads, out):
    halves, sections, rows, cols = out.shape
    block = BLOCK
    for half in range(halves):
        for i in range((cols - LANES) // block):
            piece = grads[:, (i * halves + half) * block : (i * halves + half + 1) * block]
            out[half, :, :, i * block : (i + 1) * block] = piece.reshape(sections, rows, block)
    lane = lax.broadcasted_iota(jnp.int32, (rows, LANES), 1)
    row = lax.broadcasted_iota(jnp.int32, (rows, LANES), 0)
    value = jnp.zeros((rows, LANES), jnp.float32)
    for m in range(MIXES):
        value = jnp.where(lane == m, weights[0, m], value)
    tail = jnp.zeros((rows, LANES), jnp.float32)
    for i, term in enumerate(split_terms(value)):
        tail = jnp.where(row == i, term, tail)
    tail = tail.astype(jnp.bfloat16)
    for half in range(halves):
        for k in range(sections):
            out[half, k, :, cols - LANES :] = tail


def pack_inputs_body(place, layer_in, latent, kept, sent):
    tokens, cols = kept.shape
    ranks = latent.shape[1]
    half_cols = cols - ranks - LANES
    width = layer_in.shape[1]
    block = BLOCK
    first = place[0] == 0
    squares = jnp.zeros((tokens, LANES), jnp.float32)
    for at in range(0, width, LANES):
        tile = layer_in[:, at : at + LANES].astype(jnp.float32)
        squares = squares + tile * tile
    inv_rms = lax.rsqrt(jnp.sum(squares, axis=1, keepdims=True) / width + epsilon)
    lane = lax.broadcasted_iota(jnp.int32, (tokens, LANES), 1)
    tail = jnp.zeros((tokens, LANES), jnp.float32)
    for i, term in enumerate(split_terms(jnp.broadcast_to(inv_rms, (tokens, LANES)))):
        tail = jnp.where(lane == i, term, tail)
    tail = tail.astype(jnp.bfloat16)
    for i in range(half_cols // block):
        low = layer_in[:, 2 * i * block : (2 * i + 1) * block]
        high = layer_in[:, (2 * i + 1) * block : (2 * i + 2) * block]
        kept[:, i * block : (i + 1) * block] = jnp.where(first, low, high)
        sent[:, i * block : (i + 1) * block] = jnp.where(first, high, low)
    for out in (kept, sent):
        out[:, half_cols : half_cols + ranks] = latent[...]
        out[:, half_cols + ranks :] = tail


def up_rows_body(place, up_0, up_1, up_2, up_3, out):
    turn = lax.rem(place[1] - pl.program_id(0) + 4, 4)
    near, far = (jnp.where(turn == 0, up_0[...], up_1[...]), jnp.where(turn == 2, up_2[...], up_3[...]))
    out[...] = jnp.where(turn < 2, near, far)


def lift_body(place, kept, other, kept_rest, other_rest, up_half, mixed, sends, moves, scale, act):
    del mixed
    sections, halves, rows, block = sends.shape
    ranks = up_half.shape[0]
    at = pl.program_id(0)
    first = place[0] == 0

    def in_order(own, far, half):
        return jnp.where(first, own, far) if half == 0 else jnp.where(first, far, own)

    @pl.when(at == 0)
    def _():
        for half in range(halves):
            rest = in_order(kept_rest[...], other_rest[...], half).astype(jnp.float32)
            values, slopes = gelu_pair(rest[:, :, :ranks])
            inv_rms = jnp.sum(rest[:, :, ranks : ranks + LANES], axis=2, keepdims=True)
            act[:, half] = values.astype(jnp.bfloat16)
            scale[:, half] = slopes * inv_rms

    up = up_half[...]
    for half in range(halves):
        rows_in = in_order(kept[...], other[...], half)
        moves[0, :, half, :, :block] = rows_in
        moves[0, :, half, :, block:] = act[:, half]
        branch = jnp.dot(
            act[:, half].reshape(sections * rows, ranks), up, preferred_element_type=jnp.float32
        ).reshape(sections, rows, block)
        sends[:, half] = (rows_in.astype(jnp.float32) + branch).astype(jnp.bfloat16)


def mix_body(coef, grads, out):
    halves, sections, _, cols = grads.shape
    for half in range(halves):
        for at in range(0, cols, LANES):
            lanes = slice(at, at + LANES)
            tiles = [grads[half, k, :, lanes].astype(jnp.float32) for k in range(sections)]
            for k in range(sections):
                total = coef[k, 0] * tiles[k]
                for m in range(1, sections - k):
                    total = total + coef[k, m] * tiles[k + m]
                out[k, half, :, lanes] = total.astype(jnp.bfloat16)


def gram_body(grads, outs, result):
    halves, sections, _, cols = grads.shape
    sums = {}
    for half in range(halves):
        for at in range(0, cols, LANES):
            lanes = slice(at, at + LANES)
            left = [outs[k, half, :, lanes].astype(jnp.float32) for k in range(sections)]
            right = [grads[half, k, :, lanes].astype(jnp.float32) for k in range(sections)]
            for k in range(sections):
                for m in range(sections - k):
                    product = left[k] * right[k + m]
                    folded = product[:8] + product[8:]
                    sums[k, m] = folded if (k, m) not in sums else sums[k, m] + folded

    @pl.when(pl.program_id(0) == 0)
    def _():
        result[...] = jnp.zeros(result.shape, jnp.float32)

    for (k, m), total in sums.items():
        result[k * MIXES + m] += total


def share_body(place, grads, partial, other, scale, *outs):
    sections, halves, rows, _ = grads.shape
    count = sections * halves * rows
    latent_grad = ((partial[...] + other[...].astype(jnp.float32)) * scale[...]).astype(jnp.bfloat16)
    for step, out in enumerate(outs):
        at = pl.multiple_of(lax.rem(place[1] + step, len(outs)) * BLOCK, LANES)
        out[:, :BLOCK] = grads[:, :, :, pl.ds(at, BLOCK)].reshape(count, BLOCK)
        out[:, BLOCK:] = latent_grad


def weights_body(*refs):
    half = (len(refs) - 5) // 2
    moved, shared = refs[:half], refs[half : 2 * half]
    gain, down, up_out, down_out, gain_out = refs[2 * half :]
    up_total = jnp.zeros(up_out.shape, jnp.float32)
    down_total = jnp.zeros(down_out.shape, jnp.float32)
    over_tokens = (((0,), (0,)), ((), ()))
    for left, right in zip(moved, shared):
        up_total = up_total + lax.dot_general(
            left[:, BLOCK:], right[:, :BLOCK], over_tokens, preferred_element_type=jnp.float32
        )
        down_total = down_total + lax.dot_general(
            left[:, :BLOCK], right[:, BLOCK:], over_tokens, preferred_element_type=jnp.float32
        )
    up_out[...] = up_total.astype(jnp.bfloat16)
    gain_cols = jnp.transpose(jnp.broadcast_to(gain[...].astype(jnp.float32), (8, gain.shape[1])))
    down_out[...] = (down_total * gain_cols[:, :1]).astype(jnp.bfloat16)
    product = down_total * down[...].astype(jnp.float32)
    ones = jnp.ones((8, product.shape[1]), jnp.float32)
    sums = lax.dot_general(
        ones, product, (((1,), (1,)), ((), ())), precision=lax.Precision.HIGHEST, preferred_element_type=jnp.float32
    )
    gain_out[...] = sums[:1]


def whole(layer_in, latent, mix_grad, down_proj, up_proj, norm_gain, mix_weight):
    layer_in, latent, mix_grad = (layer_in[0], latent[0], mix_grad[0])
    tokens, width = layer_in.shape
    ranks = latent.shape[1]
    xs, zs = (lax.axis_size("x"), lax.axis_size("zh"))
    sections = lax.axis_size("zl") * lax.axis_size("yh")
    block = width // (xs * zs)
    half_width = xs * block
    rows = tokens // sections
    place = jnp.stack([lax.axis_index("zh"), lax.axis_index("x")]).astype(jnp.int32)

    packed = pl.pallas_call(
        pack_grads_body,
        in_specs=[SMEM, pl.BlockSpec((tokens, width), lambda: (0, 0))],
        out_specs=pl.BlockSpec((zs, sections, rows, half_width + LANES), lambda: (0, 0, 0, 0)),
        out_shape=shape((zs, sections, rows, half_width + LANES)),
        name="pack_grads",
    )(mix_weight, mix_grad)
    grads = exchange(packed.reshape(zs * sections, rows, half_width + LANES), ("zh", *GROUP))
    grads = grads.reshape(zs, sections, rows, half_width + LANES)

    full = half_width + ranks + LANES
    kept, sent = pl.pallas_call(
        pack_inputs_body,
        in_specs=[SMEM, pl.BlockSpec((tokens, width), lambda: (0, 0)), pl.BlockSpec((tokens, ranks), lambda: (0, 0))],
        out_specs=[pl.BlockSpec((tokens, full), lambda: (0, 0))] * 2,
        out_shape=[shape((tokens, full))] * 2,
        name="pack_inputs",
    )(place, layer_in, latent)
    other = swapped(sent, "zh")

    up_block = up_proj[0]
    ups = [up_block]
    for step in range(1, xs):
        ups.append(shifted(up_block, "x", step))
    up_half = pl.pallas_call(
        up_rows_body,
        grid=(xs,),
        in_specs=[SMEM] + [pl.BlockSpec((ranks, block), lambda a: (0, 0))] * xs,
        out_specs=pl.BlockSpec((ranks, block), lambda a: (0, a)),
        out_shape=shape((ranks, half_width)),
        name="up_rows",
    )(place, *ups)

    weights = jnp.sum(grads[0, :, :TERMS, half_width : half_width + MIXES].astype(jnp.float32), axis=1)
    grads_spec = pl.BlockSpec((zs, sections, rows, block), lambda a: (0, 0, 0, a))
    chunk_spec = pl.BlockSpec((sections, zs, rows, block), lambda a: (0, 0, 0, a))
    mixed = pl.pallas_call(
        mix_body,
        grid=(xs,),
        in_specs=[SMEM, grads_spec],
        out_specs=chunk_spec,
        out_shape=shape((sections, zs, rows, half_width)),
        name="mix",
    )(weights, grads)
    arrived = exchange(mixed, GROUP)

    kept, other = [t.reshape(sections, rows, full) for t in (kept, other)]
    wide = pl.BlockSpec((sections, rows, block), lambda a: (0, 0, a))
    rest = ranks + LANES
    narrow = pl.BlockSpec((sections, rows, rest), lambda a: (0, 0, half_width // rest))
    layer_out, moves, scale = pl.pallas_call(
        lift_body,
        grid=(xs,),
        in_specs=[SMEM, wide, wide, narrow, narrow]
        + [pl.BlockSpec((ranks, block), lambda a: (0, a)), pl.BlockSpec(memory_space=pl.ANY)],
        out_specs=[
            chunk_spec,
            pl.BlockSpec((1, sections, zs, rows, block + ranks), lambda a: (a, 0, 0, 0, 0)),
            pl.BlockSpec((sections, zs, rows, ranks), lambda a: (0, 0, 0, 0)),
        ],
        out_shape=[
            shape((sections, zs, rows, half_width)),
            shape((xs, sections, zs, rows, block + ranks)),
            shape((sections, zs, rows, ranks), jnp.float32),
        ],
        scratch_shapes=[pltpu.VMEM((sections, zs, rows, ranks), jnp.bfloat16)],
        name="lift",
    )(place, kept, other, kept, other, up_half, mixed)
    scale = scale.reshape(zs * tokens, ranks)

    moves = moves.reshape(xs, zs * tokens, block + ranks)
    at_x = place[1]
    moved = [lax.dynamic_index_in_dim(moves, at_x, 0, False)]
    for step in range(1, xs):
        moved.append(shifted(lax.dynamic_index_in_dim(moves, (at_x + step) % xs, 0, False), "x", step))
    arrived, *moved = lax.optimization_barrier((arrived, *moved))

    layer_out, arrived = lax.optimization_barrier((layer_out, arrived))
    outs = exchange(layer_out, GROUP)

    act_partial = jnp.einsum(
        "tc,rc->tr", arrived.reshape(zs * tokens, half_width), up_half, preferred_element_type=jnp.float32
    )
    act_other = swapped(act_partial.astype(jnp.bfloat16), "zh")
    piece = shape((zs * tokens, block + ranks))
    shares = pl.pallas_call(
        share_body,
        in_specs=[SMEM] + [pl.BlockSpec(memory_space=pltpu.VMEM)] * 4,
        out_specs=[pl.BlockSpec(memory_space=pltpu.VMEM)] * xs,
        out_shape=[piece] * xs,
        name="share",
    )(place, arrived, act_partial, act_other, scale)
    shares = [shares[0]] + [shifted(shares[step], "x", step) for step in range(1, xs)]

    products = pl.pallas_call(
        gram_body,
        grid=(xs,),
        in_specs=[grads_spec, chunk_spec],
        out_specs=pl.BlockSpec((sections * MIXES, 8, LANES), lambda a: (0, 0, 0)),
        out_shape=shape((sections * MIXES, 8, LANES), jnp.float32),
        name="gram",
    )(grads, outs)
    products = jnp.sum(products, axis=(1, 2)).reshape(sections, MIXES)
    spread = jnp.broadcast_to(products[:, None], (sections, xs * zs, MIXES))
    mixing = exchange(spread.reshape(sections * xs * zs, MIXES), (*GROUP, "x", "zh")).sum(axis=0)

    up_grad, down_grad, gain_grad = pl.pallas_call(
        weights_body,
        in_specs=[pl.BlockSpec(memory_space=pltpu.VMEM)] * (2 * xs + 2),
        out_specs=[pl.BlockSpec(memory_space=pltpu.VMEM)] * 3,
        out_shape=[shape((ranks, block)), shape((block, ranks)), shape((1, block), jnp.float32)],
        name="weights",
    )(*moved, *shares, norm_gain, down_proj[0])
    return (up_grad[None], down_grad[None], gain_grad, mixing[None])


def solution(mesh):
    devices = mesh.devices.reshape(4, 2, 8, 4, 2)
    fine = Mesh(devices, ("zl", "yh", "r", "x", "zh"))
    section, dp = (("zl", "yh", "r"), ("x", "zh"))
    return jax.shard_map(
        whole,
        mesh=fine,
        in_specs=(
            P(section, dp, None),
            P(section, dp, None),
            P(section, dp, None),
            P(section, dp, None),
            P(section, None, dp),
            P(section, dp),
            P(section, None),
        ),
        out_specs=(
            P(section, None, dp),
            P(section, dp, None),
            P(section, dp),
            P(section, None),
        ),
        check_vma=False,
    )
```

```python
import jax
import jax.numpy as jnp
from jax import lax
from jax.experimental import pallas as pl
from jax.experimental.pallas import tpu as pltpu
from jax.sharding import Mesh, PartitionSpec as P


MIXES = 8
LANES = 128
BLOCK = 640
TERMS = 3
epsilon = 1e-06
root_coef = 0.7978845608028654
GROUP = ("zl", "yh")
SMEM = pl.BlockSpec(memory_space=pltpu.SMEM)


def gelu_pair(values):
    tangent = jnp.tanh(root_coef * (values + 0.044715 * values * values * values))
    result = 0.5 * values * (1.0 + tangent)
    slopes = 0.5 * (1.0 + tangent) + 0.5 * values * (1.0 - tangent * tangent) * root_coef * (
        1.0 + 3.0 * 0.044715 * values * values
    )
    return (result, slopes)


def exchange(pieces, axes):
    return lax.all_to_all(pieces, axes, split_axis=0, concat_axis=0, tiled=True)


def swapped(value, axis):
    return lax.ppermute(value, axis, [(0, 1), (1, 0)])


def shifted(value, axis, steps):
    count = lax.axis_size(axis)
    return lax.ppermute(value, axis, [(i, (i + steps) % count) for i in range(count)])


def split_terms(value):
    terms = []
    for _ in range(TERMS):
        term = value.astype(jnp.bfloat16).astype(jnp.float32)
        terms.append(term)
        value = value - term
    return terms


def shape(dims, dtype=jnp.bfloat16):
    return jax.ShapeDtypeStruct(dims, dtype)


def pack_grads_body(weights, grads, out):
    halves, sections, rows, cols = out.shape
    block = BLOCK
    for half in range(halves):
        for i in range((cols - LANES) // block):
            piece = grads[:, (i * halves + half) * block : (i * halves + half + 1) * block]
            out[half, :, :, i * block : (i + 1) * block] = piece.reshape(sections, rows, block)
    lane = lax.broadcasted_iota(jnp.int32, (rows, LANES), 1)
    row = lax.broadcasted_iota(jnp.int32, (rows, LANES), 0)
    value = jnp.zeros((rows, LANES), jnp.float32)
    for m in range(MIXES):
        value = jnp.where(lane == m, weights[0, m], value)
    tail = jnp.zeros((rows, LANES), jnp.float32)
    for i, term in enumerate(split_terms(value)):
        tail = jnp.where(row == i, term, tail)
    tail = tail.astype(jnp.bfloat16)
    for half in range(halves):
        for k in range(sections):
            out[half, k, :, cols - LANES :] = tail


def pack_inputs_body(place, layer_in, latent, kept, sent):
    tokens, cols = kept.shape
    ranks = latent.shape[1]
    half_cols = cols - ranks - LANES
    width = layer_in.shape[1]
    block = BLOCK
    first = place[0] == 0
    squares = jnp.zeros((tokens, LANES), jnp.float32)
    for at in range(0, width, LANES):
        tile = layer_in[:, at : at + LANES].astype(jnp.float32)
        squares = squares + tile * tile
    inv_rms = lax.rsqrt(jnp.sum(squares, axis=1, keepdims=True) / width + epsilon)
    lane = lax.broadcasted_iota(jnp.int32, (tokens, LANES), 1)
    tail = jnp.zeros((tokens, LANES), jnp.float32)
    for i, term in enumerate(split_terms(jnp.broadcast_to(inv_rms, (tokens, LANES)))):
        tail = jnp.where(lane == i, term, tail)
    tail = tail.astype(jnp.bfloat16)
    for i in range(half_cols // block):
        low = layer_in[:, 2 * i * block : (2 * i + 1) * block]
        high = layer_in[:, (2 * i + 1) * block : (2 * i + 2) * block]
        kept[:, i * block : (i + 1) * block] = jnp.where(first, low, high)
        sent[:, i * block : (i + 1) * block] = jnp.where(first, high, low)
    for out in (kept, sent):
        out[:, half_cols : half_cols + ranks] = latent[...]
        out[:, half_cols + ranks :] = tail


def up_rows_body(place, up_0, up_1, up_2, up_3, out):
    turn = lax.rem(place[1] - pl.program_id(0) + 4, 4)
    near, far = (jnp.where(turn == 0, up_0[...], up_1[...]), jnp.where(turn == 2, up_2[...], up_3[...]))
    out[...] = jnp.where(turn < 2, near, far)


def lift_body(place, kept, other, kept_rest, other_rest, up_half, mixed, sends, moves, scale, act):
    del mixed
    sections, halves, rows, block = sends.shape
    ranks = up_half.shape[0]
    at = pl.program_id(0)
    first = place[0] == 0

    def in_order(own, far, half):
        return jnp.where(first, own, far) if half == 0 else jnp.where(first, far, own)

    @pl.when(at == 0)
    def _():
        for half in range(halves):
            rest = in_order(kept_rest[...], other_rest[...], half).astype(jnp.float32)
            values, slopes = gelu_pair(rest[:, :, :ranks])
            inv_rms = jnp.sum(rest[:, :, ranks : ranks + LANES], axis=2, keepdims=True)
            act[:, half] = values.astype(jnp.bfloat16)
            scale[:, half] = slopes * inv_rms

    up = up_half[...]
    for half in range(halves):
        rows_in = in_order(kept[...], other[...], half)
        moves[0, :, half, :, :block] = rows_in
        moves[0, :, half, :, block:] = act[:, half]
        branch = jnp.dot(
            act[:, half].reshape(sections * rows, ranks), up, preferred_element_type=jnp.float32
        ).reshape(sections, rows, block)
        sends[:, half] = (rows_in.astype(jnp.float32) + branch).astype(jnp.bfloat16)


def mix_body(coef, grads, out):
    halves, sections, _, cols = grads.shape
    for half in range(halves):
        for at in range(0, cols, LANES):
            lanes = slice(at, at + LANES)
            tiles = [grads[half, k, :, lanes].astype(jnp.float32) for k in range(sections)]
            for k in range(sections):
                total = coef[k, 0] * tiles[k]
                for m in range(1, sections - k):
                    total = total + coef[k, m] * tiles[k + m]
                out[k, half, :, lanes] = total.astype(jnp.bfloat16)


def gram_body(grads, outs, result, kept):
    halves, sections, _, cols = grads.shape
    sums = {}
    for half in range(halves):
        for at in range(0, cols, LANES):
            lanes = slice(at, at + LANES)
            left = [outs[k, half, :, lanes].astype(jnp.float32) for k in range(sections)]
            right = [grads[half, k, :, lanes].astype(jnp.float32) for k in range(sections)]
            for k in range(sections):
                for m in range(sections - k):
                    product = left[k] * right[k + m]
                    folded = product[:8] + product[8:]
                    sums[k, m] = folded if (k, m) not in sums else sums[k, m] + folded

    last = pl.num_programs(0) - 1

    @pl.when(pl.program_id(0) == 0)
    def _():
        for (k, m), total in sums.items():
            kept[k * MIXES + m] = total

    @pl.when(pl.program_id(0) != 0)
    def _():
        for (k, m), total in sums.items():
            kept[k * MIXES + m] += total

    @pl.when(pl.program_id(0) == last)
    def _():
        lane = lax.broadcasted_iota(jnp.int32, (1, LANES), 1)
        share = result.shape[0] // sections
        for k in range(sections):
            row = jnp.zeros((1, LANES), jnp.float32)
            for m in range(sections - k):
                row = jnp.where(lane == m, jnp.sum(kept[k * MIXES + m], keepdims=True), row)
            result[k * share : (k + 1) * share] = jnp.broadcast_to(row, (share, LANES))


def share_body(place, grads, partial, other, scale, *outs):
    sections, halves, rows, _ = grads.shape
    count = sections * halves * rows
    latent_grad = ((partial[...] + other[...].astype(jnp.float32)) * scale[...]).astype(jnp.bfloat16)
    for step, out in enumerate(outs):
        at = pl.multiple_of(lax.rem(place[1] + step, len(outs)) * BLOCK, LANES)
        out[:, :BLOCK] = grads[:, :, :, pl.ds(at, BLOCK)].reshape(count, BLOCK)
        out[:, BLOCK:] = latent_grad


def weights_body(*refs):
    half = (len(refs) - 5) // 2
    moved, shared = refs[:half], refs[half : 2 * half]
    gain, down, up_out, down_out, gain_out = refs[2 * half :]
    up_total = jnp.zeros(up_out.shape, jnp.float32)
    down_total = jnp.zeros(down_out.shape, jnp.float32)
    over_tokens = (((0,), (0,)), ((), ()))
    for left, right in zip(moved, shared):
        up_total = up_total + lax.dot_general(
            left[:, BLOCK:], right[:, :BLOCK], over_tokens, preferred_element_type=jnp.float32
        )
        down_total = down_total + lax.dot_general(
            left[:, :BLOCK], right[:, BLOCK:], over_tokens, preferred_element_type=jnp.float32
        )
    up_out[...] = up_total.astype(jnp.bfloat16)
    gain_cols = jnp.transpose(jnp.broadcast_to(gain[...].astype(jnp.float32), (8, gain.shape[1])))
    down_out[...] = (down_total * gain_cols[:, :1]).astype(jnp.bfloat16)
    product = down_total * down[...].astype(jnp.float32)
    ones = jnp.ones((8, product.shape[1]), jnp.float32)
    sums = lax.dot_general(
        ones, product, (((1,), (1,)), ((), ())), precision=lax.Precision.HIGHEST, preferred_element_type=jnp.float32
    )
    gain_out[...] = sums[:1]


def whole(layer_in, latent, mix_grad, down_proj, up_proj, norm_gain, mix_weight):
    layer_in, latent, mix_grad = (layer_in[0], latent[0], mix_grad[0])
    tokens, width = layer_in.shape
    ranks = latent.shape[1]
    xs, zs = (lax.axis_size("x"), lax.axis_size("zh"))
    sections = lax.axis_size("zl") * lax.axis_size("yh")
    block = width // (xs * zs)
    half_width = xs * block
    rows = tokens // sections
    place = jnp.stack([lax.axis_index("zh"), lax.axis_index("x")]).astype(jnp.int32)

    packed = pl.pallas_call(
        pack_grads_body,
        in_specs=[SMEM, pl.BlockSpec((tokens, width), lambda: (0, 0))],
        out_specs=pl.BlockSpec((zs, sections, rows, half_width + LANES), lambda: (0, 0, 0, 0)),
        out_shape=shape((zs, sections, rows, half_width + LANES)),
        name="pack_grads",
    )(mix_weight, mix_grad)
    grads = exchange(packed.reshape(zs * sections, rows, half_width + LANES), ("zh", *GROUP))
    grads = grads.reshape(zs, sections, rows, half_width + LANES)

    full = half_width + ranks + LANES
    kept, sent = pl.pallas_call(
        pack_inputs_body,
        in_specs=[SMEM, pl.BlockSpec((tokens, width), lambda: (0, 0)), pl.BlockSpec((tokens, ranks), lambda: (0, 0))],
        out_specs=[pl.BlockSpec((tokens, full), lambda: (0, 0))] * 2,
        out_shape=[shape((tokens, full))] * 2,
        name="pack_inputs",
    )(place, layer_in, latent)
    other = swapped(sent, "zh")

    up_block = up_proj[0]
    ups = [up_block]
    for step in range(1, xs):
        ups.append(shifted(up_block, "x", step))
    up_half = pl.pallas_call(
        up_rows_body,
        grid=(xs,),
        in_specs=[SMEM] + [pl.BlockSpec((ranks, block), lambda a: (0, 0))] * xs,
        out_specs=pl.BlockSpec((ranks, block), lambda a: (0, a)),
        out_shape=shape((ranks, half_width)),
        name="up_rows",
    )(place, *ups)

    weights = jnp.sum(grads[0, :, :TERMS, half_width : half_width + MIXES].astype(jnp.float32), axis=1)
    grads_spec = pl.BlockSpec((zs, sections, rows, block), lambda a: (0, 0, 0, a))
    chunk_spec = pl.BlockSpec((sections, zs, rows, block), lambda a: (0, 0, 0, a))
    mixed = pl.pallas_call(
        mix_body,
        grid=(xs,),
        in_specs=[SMEM, grads_spec],
        out_specs=chunk_spec,
        out_shape=shape((sections, zs, rows, half_width)),
        name="mix",
    )(weights, grads)
    arrived = exchange(mixed, GROUP)

    kept, other = [t.reshape(sections, rows, full) for t in (kept, other)]
    wide = pl.BlockSpec((sections, rows, block), lambda a: (0, 0, a))
    rest = ranks + LANES
    narrow = pl.BlockSpec((sections, rows, rest), lambda a: (0, 0, half_width // rest))
    layer_out, moves, scale = pl.pallas_call(
        lift_body,
        grid=(xs,),
        in_specs=[SMEM, wide, wide, narrow, narrow]
        + [pl.BlockSpec((ranks, block), lambda a: (0, a)), pl.BlockSpec(memory_space=pl.ANY)],
        out_specs=[
            chunk_spec,
            pl.BlockSpec((1, sections, zs, rows, block + ranks), lambda a: (a, 0, 0, 0, 0)),
            pl.BlockSpec((sections, zs, rows, ranks), lambda a: (0, 0, 0, 0)),
        ],
        out_shape=[
            shape((sections, zs, rows, half_width)),
            shape((xs, sections, zs, rows, block + ranks)),
            shape((sections, zs, rows, ranks), jnp.float32),
        ],
        scratch_shapes=[pltpu.VMEM((sections, zs, rows, ranks), jnp.bfloat16)],
        name="lift",
    )(place, kept, other, kept, other, up_half, mixed)
    scale = scale.reshape(zs * tokens, ranks)

    moves = moves.reshape(xs, zs * tokens, block + ranks)
    at_x = place[1]
    moved = [lax.dynamic_index_in_dim(moves, at_x, 0, False)]
    for step in range(1, xs):
        moved.append(shifted(lax.dynamic_index_in_dim(moves, (at_x + step) % xs, 0, False), "x", step))

    layer_out, arrived = lax.optimization_barrier((layer_out, arrived))
    outs = exchange(layer_out, GROUP)

    act_partial = jnp.einsum(
        "tc,rc->tr", arrived.reshape(zs * tokens, half_width), up_half, preferred_element_type=jnp.float32
    )
    act_other = swapped(act_partial.astype(jnp.bfloat16), "zh")
    piece = shape((zs * tokens, block + ranks))
    shares = pl.pallas_call(
        share_body,
        in_specs=[SMEM] + [pl.BlockSpec(memory_space=pltpu.VMEM)] * 4,
        out_specs=[pl.BlockSpec(memory_space=pltpu.VMEM)] * xs,
        out_shape=[piece] * xs,
        name="share",
    )(place, arrived, act_partial, act_other, scale)
    shares = [shares[0]] + [shifted(shares[step], "x", step) for step in range(1, xs)]

    everyone = sections * xs * zs
    products = pl.pallas_call(
        gram_body,
        grid=(xs,),
        in_specs=[grads_spec, chunk_spec],
        out_specs=pl.BlockSpec((everyone, LANES), lambda a: (0, 0)),
        out_shape=shape((everyone, LANES), jnp.float32),
        scratch_shapes=[pltpu.VMEM((sections * MIXES, 8, LANES), jnp.float32)],
        name="gram",
    )(grads, outs)
    mixing = exchange(products, (*GROUP, "x", "zh")).sum(axis=0)[:MIXES]

    up_grad, down_grad, gain_grad = pl.pallas_call(
        weights_body,
        in_specs=[pl.BlockSpec(memory_space=pltpu.VMEM)] * (2 * xs + 2),
        out_specs=[pl.BlockSpec(memory_space=pltpu.VMEM)] * 3,
        out_shape=[shape((ranks, block)), shape((block, ranks)), shape((1, block), jnp.float32)],
        name="weights",
    )(*moved, *shares, norm_gain, down_proj[0])
    return (up_grad[None], down_grad[None], gain_grad, mixing[None])


def solution(mesh):
    devices = mesh.devices.reshape(4, 2, 8, 4, 2)
    fine = Mesh(devices, ("zl", "yh", "r", "x", "zh"))
    section, dp = (("zl", "yh", "r"), ("x", "zh"))
    return jax.shard_map(
        whole,
        mesh=fine,
        in_specs=(
            P(section, dp, None),
            P(section, dp, None),
            P(section, dp, None),
            P(section, dp, None),
            P(section, None, dp),
            P(section, dp),
            P(section, None),
        ),
        out_specs=(
            P(section, None, dp),
            P(section, dp, None),
            P(section, dp),
            P(section, None),
        ),
        check_vma=False,
    )
```

```python
import jax
import jax.numpy as jnp
from jax import lax
from jax.experimental import pallas as pl
from jax.experimental.pallas import tpu as pltpu
from jax.sharding import Mesh, PartitionSpec as P


MIXES = 8
LANES = 128
BLOCK = 640
TERMS = 3
epsilon = 1e-06
root_coef = 0.7978845608028654
GROUP = ("zl", "yh")
SMEM = pl.BlockSpec(memory_space=pltpu.SMEM)


def gelu_pair(values):
    tangent = jnp.tanh(root_coef * (values + 0.044715 * values * values * values))
    result = 0.5 * values * (1.0 + tangent)
    slopes = 0.5 * (1.0 + tangent) + 0.5 * values * (1.0 - tangent * tangent) * root_coef * (
        1.0 + 3.0 * 0.044715 * values * values
    )
    return (result, slopes)


def exchange(pieces, axes):
    return lax.all_to_all(pieces, axes, split_axis=0, concat_axis=0, tiled=True)


def swapped(value, axis):
    return lax.ppermute(value, axis, [(0, 1), (1, 0)])


def shifted(value, axis, steps):
    count = lax.axis_size(axis)
    return lax.ppermute(value, axis, [(i, (i + steps) % count) for i in range(count)])


def split_terms(value):
    terms = []
    for _ in range(TERMS):
        term = value.astype(jnp.bfloat16).astype(jnp.float32)
        terms.append(term)
        value = value - term
    return terms


def shape(dims, dtype=jnp.bfloat16):
    return jax.ShapeDtypeStruct(dims, dtype)


def pack_grads_body(weights, grads, out):
    halves, sections, rows, cols = out.shape
    block = BLOCK
    for half in range(halves):
        for i in range((cols - LANES) // block):
            piece = grads[:, (i * halves + half) * block : (i * halves + half + 1) * block]
            out[half, :, :, i * block : (i + 1) * block] = piece.reshape(sections, rows, block)
    lane = lax.broadcasted_iota(jnp.int32, (rows, LANES), 1)
    row = lax.broadcasted_iota(jnp.int32, (rows, LANES), 0)
    value = jnp.zeros((rows, LANES), jnp.float32)
    for m in range(MIXES):
        value = jnp.where(lane == m, weights[0, m], value)
    tail = jnp.zeros((rows, LANES), jnp.float32)
    for i, term in enumerate(split_terms(value)):
        tail = jnp.where(row == i, term, tail)
    tail = tail.astype(jnp.bfloat16)
    for half in range(halves):
        for k in range(sections):
            out[half, k, :, cols - LANES :] = tail


def pack_inputs_body(place, layer_in, latent, kept, sent, rest):
    tokens, half_cols = kept.shape
    ranks = latent.shape[1]
    width = layer_in.shape[1]
    block = BLOCK
    first = place[0] == 0
    squares = jnp.zeros((tokens, LANES), jnp.float32)
    for at in range(0, width, LANES):
        tile = layer_in[:, at : at + LANES].astype(jnp.float32)
        squares = squares + tile * tile
    inv_rms = lax.rsqrt(jnp.sum(squares, axis=1, keepdims=True) / width + epsilon)
    lane = lax.broadcasted_iota(jnp.int32, (tokens, LANES), 1)
    tail = jnp.zeros((tokens, LANES), jnp.float32)
    for i, term in enumerate(split_terms(jnp.broadcast_to(inv_rms, (tokens, LANES)))):
        tail = jnp.where(lane == i, term, tail)
    for i in range(half_cols // block):
        low = layer_in[:, 2 * i * block : (2 * i + 1) * block]
        high = layer_in[:, (2 * i + 1) * block : (2 * i + 2) * block]
        kept[:, i * block : (i + 1) * block] = jnp.where(first, low, high)
        sent[:, i * block : (i + 1) * block] = jnp.where(first, high, low)
    rest[:, :ranks] = latent[...]
    rest[:, ranks:] = tail.astype(jnp.bfloat16)


def up_rows_body(place, up_0, up_1, up_2, up_3, out):
    turn = lax.rem(place[1] - pl.program_id(0) + 4, 4)
    near, far = (jnp.where(turn == 0, up_0[...], up_1[...]), jnp.where(turn == 2, up_2[...], up_3[...]))
    out[...] = jnp.where(turn < 2, near, far)


def lift_body(place, kept, other, kept_rest, other_rest, up_half, mixed, sends, moves, scale, act):
    del mixed
    sections, halves, rows, block = sends.shape
    ranks = up_half.shape[0]
    at = pl.program_id(0)
    first = place[0] == 0

    def in_order(own, far, half):
        return jnp.where(first, own, far) if half == 0 else jnp.where(first, far, own)

    @pl.when(at == 0)
    def _():
        for half in range(halves):
            rest = in_order(kept_rest[...], other_rest[...], half).astype(jnp.float32)
            values, slopes = gelu_pair(rest[:, :, :ranks])
            inv_rms = jnp.sum(rest[:, :, ranks : ranks + LANES], axis=2, keepdims=True)
            act[:, half] = values.astype(jnp.bfloat16)
            scale[:, half] = slopes * inv_rms

    up = up_half[...]
    for half in range(halves):
        rows_in = in_order(kept[...], other[...], half)
        moves[0, :, half, :, :block] = rows_in
        moves[0, :, half, :, block:] = act[:, half]
        branch = jnp.dot(
            act[:, half].reshape(sections * rows, ranks), up, preferred_element_type=jnp.float32
        ).reshape(sections, rows, block)
        sends[:, half] = (rows_in.astype(jnp.float32) + branch).astype(jnp.bfloat16)


def mix_body(coef, grads, out):
    halves, sections, _, cols = grads.shape
    for half in range(halves):
        for at in range(0, cols, LANES):
            lanes = slice(at, at + LANES)
            tiles = [grads[half, k, :, lanes].astype(jnp.float32) for k in range(sections)]
            for k in range(sections):
                total = coef[k, 0] * tiles[k]
                for m in range(1, sections - k):
                    total = total + coef[k, m] * tiles[k + m]
                out[k, half, :, lanes] = total.astype(jnp.bfloat16)


def gram_body(grads, outs, result, kept):
    halves, sections, rows, cols = grads.shape
    total = jnp.zeros(kept.shape, jnp.float32)
    for half in range(halves):
        total = total + lax.dot_general(
            outs[:, half].reshape(sections * rows, cols),
            grads[half].reshape(sections * rows, cols),
            (((1,), (1,)), ((), ())),
            preferred_element_type=jnp.float32,
        )

    @pl.when(pl.program_id(0) == 0)
    def _():
        kept[...] = total

    @pl.when(pl.program_id(0) != 0)
    def _():
        kept[...] += total

    @pl.when(pl.program_id(0) == pl.num_programs(0) - 1)
    def _():
        row = lax.broadcasted_iota(jnp.int32, kept.shape, 0)
        lane = lax.broadcasted_iota(jnp.int32, kept.shape, 1)
        same = jnp.where(lax.rem(row, rows) == lax.rem(lane, rows), kept[...], 0.0)
        share = result.shape[0] // sections
        spread = []
        for k in range(sections):
            sums = jnp.sum(same[k * rows : (k + 1) * rows], axis=0, keepdims=True)
            sums = jnp.broadcast_to(sums, (share, LANES))
            if k:
                sums = pltpu.roll(sums, LANES - k * rows, 1)
                sums = jnp.where(lane[:share] < LANES - k * rows, sums, 0.0)
            spread.append(sums)
        gather = jnp.where(lax.div(row, rows) == lane, 1.0, 0.0)
        result[...] = jnp.dot(
            jnp.concatenate(spread, axis=0),
            gather,
            precision=lax.Precision.HIGHEST,
            preferred_element_type=jnp.float32,
        )


def share_body(place, grads, partial, other, scale, *outs):
    sections, halves, rows, _ = grads.shape
    count = sections * halves * rows
    latent_grad = ((partial[...] + other[...].astype(jnp.float32)) * scale[...]).astype(jnp.bfloat16)
    for step, out in enumerate(outs):
        at = pl.multiple_of(lax.rem(place[1] + step, len(outs)) * BLOCK, LANES)
        out[:, :BLOCK] = grads[:, :, :, pl.ds(at, BLOCK)].reshape(count, BLOCK)
        out[:, BLOCK:] = latent_grad


def weights_body(*refs):
    half = (len(refs) - 5) // 2
    moved, shared = refs[:half], refs[half : 2 * half]
    gain, down, up_out, down_out, gain_out = refs[2 * half :]
    up_total = jnp.zeros(up_out.shape, jnp.float32)
    down_total = jnp.zeros(down_out.shape, jnp.float32)
    over_tokens = (((0,), (0,)), ((), ()))
    for left, right in zip(moved, shared):
        up_total = up_total + lax.dot_general(
            left[:, BLOCK:], right[:, :BLOCK], over_tokens, preferred_element_type=jnp.float32
        )
        down_total = down_total + lax.dot_general(
            left[:, :BLOCK], right[:, BLOCK:], over_tokens, preferred_element_type=jnp.float32
        )
    up_out[...] = up_total.astype(jnp.bfloat16)
    gain_cols = jnp.transpose(jnp.broadcast_to(gain[...].astype(jnp.float32), (8, gain.shape[1])))
    down_out[...] = (down_total * gain_cols[:, :1]).astype(jnp.bfloat16)
    product = down_total * down[...].astype(jnp.float32)
    ones = jnp.ones((8, product.shape[1]), jnp.float32)
    sums = lax.dot_general(
        ones, product, (((1,), (1,)), ((), ())), precision=lax.Precision.HIGHEST, preferred_element_type=jnp.float32
    )
    gain_out[...] = sums[:1]


def whole(layer_in, latent, mix_grad, down_proj, up_proj, norm_gain, mix_weight):
    layer_in, latent, mix_grad = (layer_in[0], latent[0], mix_grad[0])
    tokens, width = layer_in.shape
    ranks = latent.shape[1]
    xs, zs = (lax.axis_size("x"), lax.axis_size("zh"))
    sections = lax.axis_size("zl") * lax.axis_size("yh")
    block = width // (xs * zs)
    half_width = xs * block
    rows = tokens // sections
    place = jnp.stack([lax.axis_index("zh"), lax.axis_index("x")]).astype(jnp.int32)

    packed = pl.pallas_call(
        pack_grads_body,
        grid=(4,),
        in_specs=[SMEM, pl.BlockSpec((tokens // 4, width), lambda i: (i, 0))],
        out_specs=pl.BlockSpec((zs, sections // 4, rows, half_width + LANES), lambda i: (0, i, 0, 0)),
        out_shape=shape((zs, sections, rows, half_width + LANES)),
        name="pack_grads",
    )(mix_weight, mix_grad)
    grads = exchange(packed.reshape(zs * sections, rows, half_width + LANES), ("zh", *GROUP))
    grads = grads.reshape(zs, sections, rows, half_width + LANES)

    rest = ranks + LANES
    kept, sent, kept_rest = pl.pallas_call(
        pack_inputs_body,
        in_specs=[SMEM, pl.BlockSpec((tokens, width), lambda: (0, 0)), pl.BlockSpec((tokens, ranks), lambda: (0, 0))],
        out_specs=[pl.BlockSpec((tokens, half_width), lambda: (0, 0))] * 2
        + [pl.BlockSpec((tokens, rest), lambda: (0, 0))],
        out_shape=[shape((tokens, half_width))] * 2 + [shape((tokens, rest))],
        name="pack_inputs",
    )(place, layer_in, latent)
    other_rest = swapped(kept_rest, "zh")
    other = swapped(sent, "zh")

    up_block = up_proj[0]
    ups = [up_block]
    for step in range(1, xs):
        ups.append(shifted(up_block, "x", step))
    up_half = pl.pallas_call(
        up_rows_body,
        grid=(xs,),
        in_specs=[SMEM] + [pl.BlockSpec((ranks, block), lambda a: (0, 0))] * xs,
        out_specs=pl.BlockSpec((ranks, block), lambda a: (0, a)),
        out_shape=shape((ranks, half_width)),
        name="up_rows",
    )(place, *ups)

    weights = jnp.sum(grads[0, :, :TERMS, half_width : half_width + MIXES].astype(jnp.float32), axis=1)
    grads_spec = pl.BlockSpec((zs, sections, rows, block), lambda a: (0, 0, 0, a))
    chunk_spec = pl.BlockSpec((sections, zs, rows, block), lambda a: (0, 0, 0, a))
    mixed = pl.pallas_call(
        mix_body,
        grid=(xs,),
        in_specs=[SMEM, grads_spec],
        out_specs=chunk_spec,
        out_shape=shape((sections, zs, rows, half_width)),
        name="mix",
    )(weights, grads)
    arrived = exchange(mixed, GROUP)

    kept, other, kept_rest, other_rest = [
        t.reshape(sections, rows, t.shape[1]) for t in (kept, other, kept_rest, other_rest)
    ]
    wide = pl.BlockSpec((sections, rows, block), lambda a: (0, 0, a))
    narrow = pl.BlockSpec((sections, rows, rest), lambda a: (0, 0, 0))
    layer_out, moves, scale = pl.pallas_call(
        lift_body,
        grid=(xs,),
        in_specs=[SMEM, wide, wide, narrow, narrow]
        + [pl.BlockSpec((ranks, block), lambda a: (0, a)), pl.BlockSpec(memory_space=pl.ANY)],
        out_specs=[
            chunk_spec,
            pl.BlockSpec((1, sections, zs, rows, block + ranks), lambda a: (a, 0, 0, 0, 0)),
            pl.BlockSpec((sections, zs, rows, ranks), lambda a: (0, 0, 0, 0)),
        ],
        out_shape=[
            shape((sections, zs, rows, half_width)),
            shape((xs, sections, zs, rows, block + ranks)),
            shape((sections, zs, rows, ranks), jnp.float32),
        ],
        scratch_shapes=[pltpu.VMEM((sections, zs, rows, ranks), jnp.bfloat16)],
        name="lift",
    )(place, kept, other, kept_rest, other_rest, up_half, mixed)
    scale = scale.reshape(zs * tokens, ranks)

    moves = moves.reshape(xs, zs * tokens, block + ranks)
    at_x = place[1]
    moved = [lax.dynamic_index_in_dim(moves, at_x, 0, False)]
    for step in range(1, xs):
        moved.append(shifted(lax.dynamic_index_in_dim(moves, (at_x + step) % xs, 0, False), "x", step))

    layer_out, arrived = lax.optimization_barrier((layer_out, arrived))
    outs = exchange(layer_out, GROUP)

    act_partial = jnp.einsum(
        "tc,rc->tr", arrived.reshape(zs * tokens, half_width), up_half, preferred_element_type=jnp.float32
    )
    act_other = swapped(act_partial.astype(jnp.bfloat16), "zh")
    piece = shape((zs * tokens, block + ranks))
    shares = pl.pallas_call(
        share_body,
        in_specs=[SMEM] + [pl.BlockSpec(memory_space=pltpu.VMEM)] * 4,
        out_specs=[pl.BlockSpec(memory_space=pltpu.VMEM)] * xs,
        out_shape=[piece] * xs,
        name="share",
    )(place, arrived, act_partial, act_other, scale)
    shares = list(shares)
    for step in range(1, xs):
        shares[step] = shifted(shares[step], "x", step)

    everyone = sections * xs * zs
    products = pl.pallas_call(
        gram_body,
        grid=(xs,),
        in_specs=[grads_spec, chunk_spec],
        out_specs=pl.BlockSpec((everyone, LANES), lambda a: (0, 0)),
        out_shape=shape((everyone, LANES), jnp.float32),
        scratch_shapes=[pltpu.VMEM((sections * rows, LANES), jnp.float32)],
        name="gram",
    )(grads, outs)
    mixing = exchange(products, (*GROUP, "x", "zh")).sum(axis=0)[:MIXES]

    up_grad, down_grad, gain_grad = pl.pallas_call(
        weights_body,
        in_specs=[pl.BlockSpec(memory_space=pltpu.VMEM)] * (2 * xs + 2),
        out_specs=[pl.BlockSpec(memory_space=pltpu.VMEM)] * 3,
        out_shape=[shape((ranks, block)), shape((block, ranks)), shape((1, block), jnp.float32)],
        name="weights",
    )(*moved, *shares, norm_gain, down_proj[0])
    return (up_grad[None], down_grad[None], gain_grad, mixing[None])


def solution(mesh):
    devices = mesh.devices.reshape(4, 2, 8, 4, 2)
    fine = Mesh(devices, ("zl", "yh", "r", "x", "zh"))
    section, dp = (("zl", "yh", "r"), ("x", "zh"))
    return jax.shard_map(
        whole,
        mesh=fine,
        in_specs=(
            P(section, dp, None),
            P(section, dp, None),
            P(section, dp, None),
            P(section, dp, None),
            P(section, None, dp),
            P(section, dp),
            P(section, None),
        ),
        out_specs=(
            P(section, None, dp),
            P(section, dp, None),
            P(section, dp),
            P(section, None),
        ),
        check_vma=False,
    )
```

```python
import jax
import jax.numpy as jnp
from jax import lax
from jax.experimental import pallas as pl
from jax.experimental.pallas import tpu as pltpu
from jax.sharding import Mesh, PartitionSpec as P


MIXES = 8
LANES = 128
BLOCK = 640
TERMS = 3
epsilon = 1e-06
root_coef = 0.7978845608028654
GROUP = ("zl", "yh")
SMEM = pl.BlockSpec(memory_space=pltpu.SMEM)
VMEM = pl.BlockSpec(memory_space=pltpu.VMEM)


def gelu_pair(values):
    tangent = jnp.tanh(root_coef * (values + 0.044715 * values * values * values))
    result = 0.5 * values * (1.0 + tangent)
    slopes = 0.5 * (1.0 + tangent) + 0.5 * values * (1.0 - tangent * tangent) * root_coef * (
        1.0 + 3.0 * 0.044715 * values * values
    )
    return (result, slopes)


def exchange(pieces, axes):
    return lax.all_to_all(pieces, axes, split_axis=0, concat_axis=0, tiled=True)


def swapped(value, axis):
    return lax.ppermute(value, axis, [(0, 1), (1, 0)])


def shifted(value, axis, steps):
    count = lax.axis_size(axis)
    return lax.ppermute(value, axis, [(i, (i + steps) % count) for i in range(count)])


def split_terms(value):
    terms = []
    for _ in range(TERMS):
        term = value.astype(jnp.bfloat16).astype(jnp.float32)
        terms.append(term)
        value = value - term
    return terms


def shape(dims, dtype=jnp.bfloat16):
    return jax.ShapeDtypeStruct(dims, dtype)


def pack_grads_body(weights, grads, out):
    halves, sections, rows, cols = out.shape
    block = BLOCK
    for half in range(halves):
        for i in range((cols - LANES) // block):
            piece = grads[:, (i * halves + half) * block : (i * halves + half + 1) * block]
            out[half, :, :, i * block : (i + 1) * block] = piece.reshape(sections, rows, block)
    lane = lax.broadcasted_iota(jnp.int32, (rows, LANES), 1)
    row = lax.broadcasted_iota(jnp.int32, (rows, LANES), 0)
    value = jnp.zeros((rows, LANES), jnp.float32)
    for m in range(MIXES):
        value = jnp.where(lane == m, weights[0, m], value)
    tail = jnp.zeros((rows, LANES), jnp.float32)
    for i, term in enumerate(split_terms(value)):
        tail = jnp.where(row == i, term, tail)
    tail = tail.astype(jnp.bfloat16)
    for half in range(halves):
        for k in range(sections):
            out[half, k, :, cols - LANES :] = tail


def pack_inputs_body(place, layer_in, latent, kept, sent, rest):
    tokens, half_cols = kept.shape
    ranks = latent.shape[1]
    width = layer_in.shape[1]
    block = BLOCK
    first = place[0] == 0
    squares = jnp.zeros((tokens, LANES), jnp.float32)
    for at in range(0, width, LANES):
        tile = layer_in[:, at : at + LANES].astype(jnp.float32)
        squares = squares + tile * tile
    inv_rms = lax.rsqrt(jnp.sum(squares, axis=1, keepdims=True) / width + epsilon)
    lane = lax.broadcasted_iota(jnp.int32, (tokens, LANES), 1)
    tail = jnp.zeros((tokens, LANES), jnp.float32)
    for i, term in enumerate(split_terms(jnp.broadcast_to(inv_rms, (tokens, LANES)))):
        tail = jnp.where(lane == i, term, tail)
    for i in range(half_cols // block):
        low = layer_in[:, 2 * i * block : (2 * i + 1) * block]
        high = layer_in[:, (2 * i + 1) * block : (2 * i + 2) * block]
        kept[:, i * block : (i + 1) * block] = jnp.where(first, low, high)
        sent[:, i * block : (i + 1) * block] = jnp.where(first, high, low)
    rest[:, :ranks] = latent[...]
    rest[:, ranks:] = tail.astype(jnp.bfloat16)


def activate_body(place, kept, other, up, act, scale, out):
    sections, halves, rows, ranks = act.shape
    first = place[0] == 0
    for half in range(halves):
        near, far = (kept[...], other[...]) if half == 0 else (other[...], kept[...])
        rest = jnp.where(first, near, far).astype(jnp.float32)
        values, slopes = gelu_pair(rest[:, :, :ranks])
        inv_rms = jnp.sum(rest[:, :, ranks:], axis=2, keepdims=True)
        act[:, half] = values.astype(jnp.bfloat16)
        scale[:, half] = slopes * inv_rms
    out[:, :BLOCK] = up[...]
    whole_act = act[...].reshape(sections * halves * rows, ranks).astype(jnp.float32)
    out[:, BLOCK:] = jnp.transpose(whole_act).astype(jnp.bfloat16)


def up_rows_body(place, up_0, up_1, up_2, up_3, out):
    for i in range(4):
        turn = lax.rem(place[1] - i + 4, 4)
        pieces = [up[:, :BLOCK] for up in (up_0, up_1, up_2, up_3)]
        near, far = (jnp.where(turn == 0, pieces[0], pieces[1]), jnp.where(turn == 2, pieces[2], pieces[3]))
        out[:, i * BLOCK : (i + 1) * BLOCK] = jnp.where(turn < 2, near, far)


def lift_body(place, kept, other, act, up_half, mixed, sends, inputs):
    del mixed
    sections, halves, rows, width = sends.shape
    ranks = up_half.shape[0]
    first = place[0] == 0
    for at in range(0, width, BLOCK):
        lanes = slice(at, at + BLOCK)
        for half in range(halves):
            near, far = (kept, other) if half == 0 else (other, kept)
            rows_in = jnp.where(first, near[:, :, lanes], far[:, :, lanes])
            inputs[:, half, :, lanes] = rows_in
            branch = jnp.dot(
                act[:, half].reshape(sections * rows, ranks), up_half[:, lanes], preferred_element_type=jnp.float32
            ).reshape(sections, rows, BLOCK)
            sends[:, half, :, lanes] = (rows_in.astype(jnp.float32) + branch).astype(jnp.bfloat16)


def mix_body(coef, grads, out):
    sections, halves, _, cols = out.shape
    for half in range(halves):
        for at in range(0, cols, LANES):
            lanes = slice(at, at + LANES)
            tiles = [grads[half, k, :, lanes].astype(jnp.float32) for k in range(sections)]
            for k in range(sections):
                total = coef[k, 0] * tiles[k]
                for m in range(1, sections - k):
                    total = total + coef[k, m] * tiles[k + m]
                out[k, half, :, lanes] = total.astype(jnp.bfloat16)


def gram_body(grads, outs, result):
    sections, halves, rows, cols = outs.shape
    total = jnp.zeros((sections * rows, LANES), jnp.float32)
    for half in range(halves):
        total = total + lax.dot_general(
            outs[:, half].reshape(sections * rows, cols),
            grads[half, :, :, :cols].reshape(sections * rows, cols),
            (((1,), (1,)), ((), ())),
            preferred_element_type=jnp.float32,
        )
    row = lax.broadcasted_iota(jnp.int32, total.shape, 0)
    lane = lax.broadcasted_iota(jnp.int32, total.shape, 1)
    same = jnp.where(lax.rem(row, rows) == lax.rem(lane, rows), total, 0.0)
    share = result.shape[0] // sections
    spread = []
    for k in range(sections):
        sums = jnp.sum(same[k * rows : (k + 1) * rows], axis=0, keepdims=True)
        sums = jnp.broadcast_to(sums, (share, LANES))
        if k:
            sums = pltpu.roll(sums, LANES - k * rows, 1)
            sums = jnp.where(lane[:share] < LANES - k * rows, sums, 0.0)
        spread.append(sums)
    gather = jnp.where(lax.div(row, rows) == lane, 1.0, 0.0)
    result[...] = jnp.dot(
        jnp.concatenate(spread, axis=0), gather, precision=lax.Precision.HIGHEST, preferred_element_type=jnp.float32
    )


def share_body(place, inputs, grads, partial, other, scale, *outs):
    sections, halves, rows, _ = grads.shape
    count = sections * halves * rows
    latent_grad = ((partial[...] + other[...].astype(jnp.float32)) * scale[...]).astype(jnp.bfloat16)
    for step, out in enumerate(outs):
        at = pl.multiple_of(lax.rem(place[1] + step, len(outs)) * BLOCK, LANES)
        out[:, :BLOCK] = inputs[:, :, :, pl.ds(at, BLOCK)].reshape(count, BLOCK)
        out[:, BLOCK : 2 * BLOCK] = grads[:, :, :, pl.ds(at, BLOCK)].reshape(count, BLOCK)
        out[:, 2 * BLOCK :] = latent_grad


def weights_body(*refs):
    half = (len(refs) - 5) // 2
    acts, shared = refs[:half], refs[half : 2 * half]
    gain, down, up_out, down_out, gain_out = refs[2 * half :]
    up_total = jnp.zeros(up_out.shape, jnp.float32)
    down_total = jnp.zeros(down_out.shape, jnp.float32)
    for act, piece in zip(acts, shared):
        up_total = up_total + jnp.dot(
            act[:, BLOCK:], piece[:, BLOCK : 2 * BLOCK], preferred_element_type=jnp.float32
        )
        down_total = down_total + lax.dot_general(
            piece[:, :BLOCK], piece[:, 2 * BLOCK :], (((0,), (0,)), ((), ())), preferred_element_type=jnp.float32
        )
    up_out[...] = up_total.astype(jnp.bfloat16)
    gain_cols = jnp.transpose(jnp.broadcast_to(gain[...].astype(jnp.float32), (8, gain.shape[1])))
    down_out[...] = (down_total * gain_cols[:, :1]).astype(jnp.bfloat16)
    product = down_total * down[...].astype(jnp.float32)
    ones = jnp.ones((8, product.shape[1]), jnp.float32)
    sums = lax.dot_general(
        ones, product, (((1,), (1,)), ((), ())), precision=lax.Precision.HIGHEST, preferred_element_type=jnp.float32
    )
    gain_out[...] = sums[:1]


def whole(layer_in, latent, mix_grad, down_proj, up_proj, norm_gain, mix_weight):
    layer_in, latent, mix_grad = (layer_in[0], latent[0], mix_grad[0])
    tokens, width = layer_in.shape
    ranks = latent.shape[1]
    xs, zs = (lax.axis_size("x"), lax.axis_size("zh"))
    sections = lax.axis_size("zl") * lax.axis_size("yh")
    block = width // (xs * zs)
    half_width = xs * block
    rows = tokens // sections
    place = jnp.stack([lax.axis_index("zh"), lax.axis_index("x")]).astype(jnp.int32)

    packed = pl.pallas_call(
        pack_grads_body,
        in_specs=[SMEM, pl.BlockSpec((tokens, width), lambda: (0, 0))],
        out_specs=pl.BlockSpec((zs, sections, rows, half_width + LANES), lambda: (0, 0, 0, 0)),
        out_shape=shape((zs, sections, rows, half_width + LANES)),
        name="pack_grads",
    )(mix_weight, mix_grad)
    grads = exchange(packed.reshape(zs * sections, rows, half_width + LANES), ("zh", *GROUP))
    grads = grads.reshape(zs, sections, rows, half_width + LANES)

    rest = ranks + LANES
    kept, sent, kept_rest = pl.pallas_call(
        pack_inputs_body,
        in_specs=[SMEM, pl.BlockSpec((tokens, width), lambda: (0, 0)), pl.BlockSpec((tokens, ranks), lambda: (0, 0))],
        out_specs=[pl.BlockSpec((tokens, half_width), lambda: (0, 0))] * 2
        + [pl.BlockSpec((tokens, rest), lambda: (0, 0))],
        out_shape=[shape((tokens, half_width))] * 2 + [shape((tokens, rest))],
        name="pack_inputs",
    )(place, layer_in, latent)
    other_rest = swapped(kept_rest, "zh")
    other = swapped(sent, "zh")

    kept, other, kept_rest, other_rest = [
        t.reshape(sections, rows, t.shape[1]) for t in (kept, other, kept_rest, other_rest)
    ]
    act, scale, up_part = pl.pallas_call(
        activate_body,
        in_specs=[SMEM] + [VMEM] * 3,
        out_specs=[VMEM] * 3,
        out_shape=[
            shape((sections, zs, rows, ranks)),
            shape((sections, zs, rows, ranks), jnp.float32),
            shape((ranks, block + zs * tokens)),
        ],
        name="activate",
    )(place, kept_rest, other_rest, up_proj[0])
    scale = scale.reshape(zs * tokens, ranks)

    ups = [up_part]
    for step in range(1, xs):
        ups.append(shifted(up_part, "x", step))
    up_half = pl.pallas_call(
        up_rows_body,
        in_specs=[SMEM] + [VMEM] * xs,
        out_specs=VMEM,
        out_shape=shape((ranks, half_width)),
        name="up_rows",
    )(place, *ups)

    weights = jnp.sum(grads[0, :, :TERMS, half_width : half_width + MIXES].astype(jnp.float32), axis=1)
    chunk = shape((sections, zs, rows, half_width))
    mixed = pl.pallas_call(mix_body, in_specs=[SMEM, VMEM], out_specs=VMEM, out_shape=chunk, name="mix")(weights, grads)
    arrived = exchange(mixed, GROUP)

    layer_out, inputs = pl.pallas_call(
        lift_body,
        in_specs=[SMEM] + [VMEM] * 4 + [pl.BlockSpec(memory_space=pl.ANY)],
        out_specs=[VMEM] * 2,
        out_shape=[chunk] * 2,
        name="lift",
    )(place, kept, other, act, up_half, mixed)

    layer_out, arrived = lax.optimization_barrier((layer_out, arrived))
    outs = exchange(layer_out, GROUP)

    act_partial = jnp.einsum(
        "tc,rc->tr", arrived.reshape(zs * tokens, half_width), up_half, preferred_element_type=jnp.float32
    )
    act_other = swapped(act_partial.astype(jnp.bfloat16), "zh")
    shares = pl.pallas_call(
        share_body,
        in_specs=[SMEM] + [VMEM] * 5,
        out_specs=[VMEM] * xs,
        out_shape=[shape((zs * tokens, 2 * block + ranks))] * xs,
        name="share",
    )(place, inputs, arrived, act_partial, act_other, scale)
    shares = list(shares)
    for step in range(1, xs):
        shares[step] = shifted(shares[step], "x", step)

    everyone = sections * xs * zs
    products = pl.pallas_call(
        gram_body,
        in_specs=[VMEM] * 2,
        out_specs=VMEM,
        out_shape=shape((everyone, LANES), jnp.float32),
        name="gram",
    )(grads, outs)
    mixing = exchange(products, (*GROUP, "x", "zh")).sum(axis=0)[:MIXES]

    up_grad, down_grad, gain_grad = pl.pallas_call(
        weights_body,
        in_specs=[VMEM] * (2 * xs + 2),
        out_specs=[VMEM] * 3,
        out_shape=[shape((ranks, block)), shape((block, ranks)), shape((1, block), jnp.float32)],
        name="weights",
    )(*ups, *shares, norm_gain, down_proj[0])
    return (up_grad[None], down_grad[None], gain_grad, mixing[None])


def solution(mesh):
    devices = mesh.devices.reshape(4, 2, 8, 4, 2)
    fine = Mesh(devices, ("zl", "yh", "r", "x", "zh"))
    section, dp = (("zl", "yh", "r"), ("x", "zh"))
    return jax.shard_map(
        whole,
        mesh=fine,
        in_specs=(
            P(section, dp, None),
            P(section, dp, None),
            P(section, dp, None),
            P(section, dp, None),
            P(section, None, dp),
            P(section, dp),
            P(section, None),
        ),
        out_specs=(
            P(section, None, dp),
            P(section, dp, None),
            P(section, dp),
            P(section, None),
        ),
        check_vma=False,
    )
```

```python
import jax
import jax.numpy as jnp
from jax import lax
from jax.experimental import pallas as pl
from jax.experimental.pallas import tpu as pltpu
from jax.sharding import Mesh, PartitionSpec as P


MIXES = 8
LANES = 128
BLOCK = 640
TERMS = 3
epsilon = 1e-06
root_coef = 0.7978845608028654
GROUP = ("zl", "yh")
SMEM = pl.BlockSpec(memory_space=pltpu.SMEM)
VMEM = pl.BlockSpec(memory_space=pltpu.VMEM)


def gelu_pair(values):
    tangent = jnp.tanh(root_coef * (values + 0.044715 * values * values * values))
    result = 0.5 * values * (1.0 + tangent)
    slopes = 0.5 * (1.0 + tangent) + 0.5 * values * (1.0 - tangent * tangent) * root_coef * (
        1.0 + 3.0 * 0.044715 * values * values
    )
    return (result, slopes)


def exchange(pieces, axes):
    return lax.all_to_all(pieces, axes, split_axis=0, concat_axis=0, tiled=True)


def swapped(value, axis):
    return lax.ppermute(value, axis, [(0, 1), (1, 0)])


def shifted(value, axis, steps):
    count = lax.axis_size(axis)
    return lax.ppermute(value, axis, [(i, (i + steps) % count) for i in range(count)])


def split_terms(value):
    terms = []
    for _ in range(TERMS):
        term = value.astype(jnp.bfloat16).astype(jnp.float32)
        terms.append(term)
        value = value - term
    return terms


def shape(dims, dtype=jnp.bfloat16):
    return jax.ShapeDtypeStruct(dims, dtype)


def pack_grads_body(weights, grads, out):
    halves, sections, rows, cols = out.shape
    block = BLOCK
    for half in range(halves):
        for i in range((cols - LANES) // block):
            piece = grads[:, (i * halves + half) * block : (i * halves + half + 1) * block]
            out[half, :, :, i * block : (i + 1) * block] = piece.reshape(sections, rows, block)
    lane = lax.broadcasted_iota(jnp.int32, (rows, LANES), 1)
    row = lax.broadcasted_iota(jnp.int32, (rows, LANES), 0)
    value = jnp.zeros((rows, LANES), jnp.float32)
    for m in range(MIXES):
        value = jnp.where(lane == m, weights[0, m], value)
    tail = jnp.zeros((rows, LANES), jnp.float32)
    for i, term in enumerate(split_terms(value)):
        tail = jnp.where(row == i, term, tail)
    tail = tail.astype(jnp.bfloat16)
    for half in range(halves):
        for k in range(sections):
            out[half, k, :, cols - LANES :] = tail


def pack_inputs_body(place, layer_in, kept, sent):
    tokens, cols = kept.shape
    half_cols = cols - LANES
    width = layer_in.shape[1]
    block = BLOCK
    first = place[0] == 0
    squares = jnp.zeros((tokens, LANES), jnp.float32)
    for at in range(0, width, LANES):
        tile = layer_in[:, at : at + LANES].astype(jnp.float32)
        squares = squares + tile * tile
    inv_rms = lax.rsqrt(jnp.sum(squares, axis=1, keepdims=True) / width + epsilon)
    lane = lax.broadcasted_iota(jnp.int32, (tokens, LANES), 1)
    tail = jnp.zeros((tokens, LANES), jnp.float32)
    for i, term in enumerate(split_terms(jnp.broadcast_to(inv_rms, (tokens, LANES)))):
        tail = jnp.where(lane == i, term, tail)
    for i in range(half_cols // block):
        low = layer_in[:, 2 * i * block : (2 * i + 1) * block]
        high = layer_in[:, (2 * i + 1) * block : (2 * i + 2) * block]
        kept[:, i * block : (i + 1) * block] = jnp.where(first, low, high)
        sent[:, i * block : (i + 1) * block] = jnp.where(first, high, low)
    tail = tail.astype(jnp.bfloat16)
    kept[:, half_cols:] = tail
    sent[:, half_cols:] = tail


def activate_body(place, kept, other, up, act, slopes_out, out):
    sections, halves, rows, ranks = act.shape
    first = place[0] == 0
    for half in range(halves):
        near, far = (kept[...], other[...]) if half == 0 else (other[...], kept[...])
        values, slopes = gelu_pair(jnp.where(first, near, far).astype(jnp.float32))
        act[:, half] = values.astype(jnp.bfloat16)
        slopes_out[:, half] = slopes
    out[:, :BLOCK] = up[...]
    whole_act = act[...].reshape(sections * halves * rows, ranks).astype(jnp.float32)
    out[:, BLOCK:] = jnp.transpose(whole_act).astype(jnp.bfloat16)


def up_rows_body(place, up_0, up_1, up_2, up_3, out):
    for i in range(4):
        turn = lax.rem(place[1] - i + 4, 4)
        pieces = [up[:, :BLOCK] for up in (up_0, up_1, up_2, up_3)]
        near, far = (jnp.where(turn == 0, pieces[0], pieces[1]), jnp.where(turn == 2, pieces[2], pieces[3]))
        out[:, i * BLOCK : (i + 1) * BLOCK] = jnp.where(turn < 2, near, far)


def lift_body(place, kept, other, act, slopes, up_half, mixed, sends, inputs, scale):
    del mixed
    sections, halves, rows, width = sends.shape
    ranks = up_half.shape[0]
    first = place[0] == 0
    for half in range(halves):
        near, far = (kept, other) if half == 0 else (other, kept)
        terms = jnp.where(first, near[:, :, width:], far[:, :, width:]).astype(jnp.float32)
        scale[:, half] = slopes[:, half] * jnp.sum(terms, axis=2, keepdims=True)
    for at in range(0, width, BLOCK):
        lanes = slice(at, at + BLOCK)
        for half in range(halves):
            near, far = (kept, other) if half == 0 else (other, kept)
            rows_in = jnp.where(first, near[:, :, lanes], far[:, :, lanes])
            inputs[:, half, :, lanes] = rows_in
            branch = jnp.dot(
                act[:, half].reshape(sections * rows, ranks), up_half[:, lanes], preferred_element_type=jnp.float32
            ).reshape(sections, rows, BLOCK)
            sends[:, half, :, lanes] = (rows_in.astype(jnp.float32) + branch).astype(jnp.bfloat16)


def mix_body(coef, grads, out):
    sections, halves, _, cols = out.shape
    for half in range(halves):
        for at in range(0, cols, LANES):
            lanes = slice(at, at + LANES)
            tiles = [grads[half, k, :, lanes].astype(jnp.float32) for k in range(sections)]
            for k in range(sections):
                total = coef[k, 0] * tiles[k]
                for m in range(1, sections - k):
                    total = total + coef[k, m] * tiles[k + m]
                out[k, half, :, lanes] = total.astype(jnp.bfloat16)


def gram_body(grads, outs, result):
    sections, halves, rows, cols = outs.shape
    total = jnp.zeros((sections * rows, LANES), jnp.float32)
    for half in range(halves):
        total = total + lax.dot_general(
            outs[:, half].reshape(sections * rows, cols),
            grads[half, :, :, :cols].reshape(sections * rows, cols),
            (((1,), (1,)), ((), ())),
            preferred_element_type=jnp.float32,
        )
    row = lax.broadcasted_iota(jnp.int32, total.shape, 0)
    lane = lax.broadcasted_iota(jnp.int32, total.shape, 1)
    same = jnp.where(lax.rem(row, rows) == lax.rem(lane, rows), total, 0.0)
    share = result.shape[0] // sections
    spread = []
    for k in range(sections):
        sums = jnp.sum(same[k * rows : (k + 1) * rows], axis=0, keepdims=True)
        sums = jnp.broadcast_to(sums, (share, LANES))
        if k:
            sums = pltpu.roll(sums, LANES - k * rows, 1)
            sums = jnp.where(lane[:share] < LANES - k * rows, sums, 0.0)
        spread.append(sums)
    gather = jnp.where(lax.div(row, rows) == lane, 1.0, 0.0)
    result[...] = jnp.dot(
        jnp.concatenate(spread, axis=0), gather, precision=lax.Precision.HIGHEST, preferred_element_type=jnp.float32
    )


def share_body(place, inputs, grads, partial, other, scale, *outs):
    sections, halves, rows, _ = grads.shape
    count = sections * halves * rows
    latent_grad = ((partial[...] + other[...].astype(jnp.float32)) * scale[...]).astype(jnp.bfloat16)
    for step, out in enumerate(outs):
        at = pl.multiple_of(lax.rem(place[1] + step, len(outs)) * BLOCK, LANES)
        out[:, :BLOCK] = inputs[:, :, :, pl.ds(at, BLOCK)].reshape(count, BLOCK)
        out[:, BLOCK : 2 * BLOCK] = grads[:, :, :, pl.ds(at, BLOCK)].reshape(count, BLOCK)
        out[:, 2 * BLOCK :] = latent_grad


def weights_body(*refs):
    half = (len(refs) - 5) // 2
    acts, shared = refs[:half], refs[half : 2 * half]
    gain, down, up_out, down_out, gain_out = refs[2 * half :]
    up_total = jnp.zeros(up_out.shape, jnp.float32)
    down_total = jnp.zeros(down_out.shape, jnp.float32)
    for act, piece in zip(acts, shared):
        up_total = up_total + jnp.dot(
            act[:, BLOCK:], piece[:, BLOCK : 2 * BLOCK], preferred_element_type=jnp.float32
        )
        down_total = down_total + lax.dot_general(
            piece[:, :BLOCK], piece[:, 2 * BLOCK :], (((0,), (0,)), ((), ())), preferred_element_type=jnp.float32
        )
    up_out[...] = up_total.astype(jnp.bfloat16)
    gain_cols = jnp.transpose(jnp.broadcast_to(gain[...].astype(jnp.float32), (8, gain.shape[1])))
    down_out[...] = (down_total * gain_cols[:, :1]).astype(jnp.bfloat16)
    product = down_total * down[...].astype(jnp.float32)
    ones = jnp.ones((8, product.shape[1]), jnp.float32)
    sums = lax.dot_general(
        ones, product, (((1,), (1,)), ((), ())), precision=lax.Precision.HIGHEST, preferred_element_type=jnp.float32
    )
    gain_out[...] = sums[:1]


def whole(layer_in, latent, mix_grad, down_proj, up_proj, norm_gain, mix_weight):
    layer_in, latent, mix_grad = (layer_in[0], latent[0], mix_grad[0])
    tokens, width = layer_in.shape
    ranks = latent.shape[1]
    xs, zs = (lax.axis_size("x"), lax.axis_size("zh"))
    sections = lax.axis_size("zl") * lax.axis_size("yh")
    block = width // (xs * zs)
    half_width = xs * block
    rows = tokens // sections
    place = jnp.stack([lax.axis_index("zh"), lax.axis_index("x")]).astype(jnp.int32)

    packed = pl.pallas_call(
        pack_grads_body,
        in_specs=[SMEM, pl.BlockSpec((tokens, width), lambda: (0, 0))],
        out_specs=pl.BlockSpec((zs, sections, rows, half_width + LANES), lambda: (0, 0, 0, 0)),
        out_shape=shape((zs, sections, rows, half_width + LANES)),
        name="pack_grads",
    )(mix_weight, mix_grad)
    grads = exchange(packed.reshape(zs * sections, rows, half_width + LANES), ("zh", *GROUP))
    grads = grads.reshape(zs, sections, rows, half_width + LANES)

    full = half_width + LANES
    kept, sent = pl.pallas_call(
        pack_inputs_body,
        in_specs=[SMEM, pl.BlockSpec((tokens, width), lambda: (0, 0))],
        out_specs=[pl.BlockSpec((tokens, full), lambda: (0, 0))] * 2,
        out_shape=[shape((tokens, full))] * 2,
        name="pack_inputs",
    )(place, layer_in)
    other = swapped(sent, "zh")
    other_latent = swapped(latent, "zh")
    kept, other, latent, other_latent = [
        t.reshape(sections, rows, t.shape[1]) for t in (kept, other, latent, other_latent)
    ]
    act, slopes, up_part = pl.pallas_call(
        activate_body,
        in_specs=[SMEM] + [VMEM] * 3,
        out_specs=[VMEM] * 3,
        out_shape=[
            shape((sections, zs, rows, ranks)),
            shape((sections, zs, rows, ranks), jnp.float32),
            shape((ranks, block + zs * tokens)),
        ],
        name="activate",
    )(place, latent, other_latent, up_proj[0])

    ups = [up_part]
    for step in range(1, xs):
        ups.append(shifted(up_part, "x", step))
    up_half = pl.pallas_call(
        up_rows_body,
        in_specs=[SMEM] + [VMEM] * xs,
        out_specs=VMEM,
        out_shape=shape((ranks, half_width)),
        name="up_rows",
    )(place, *ups)

    weights = jnp.sum(grads[0, :, :TERMS, half_width : half_width + MIXES].astype(jnp.float32), axis=1)
    chunk = shape((sections, zs, rows, half_width))
    mixed = pl.pallas_call(mix_body, in_specs=[SMEM, VMEM], out_specs=VMEM, out_shape=chunk, name="mix")(weights, grads)
    arrived = exchange(mixed, GROUP)

    layer_out, inputs, scale = pl.pallas_call(
        lift_body,
        in_specs=[SMEM] + [VMEM] * 5 + [pl.BlockSpec(memory_space=pl.ANY)],
        out_specs=[VMEM] * 3,
        out_shape=[chunk] * 2 + [shape((sections, zs, rows, ranks), jnp.float32)],
        name="lift",
    )(place, kept, other, act, slopes, up_half, mixed)
    scale = scale.reshape(zs * tokens, ranks)

    layer_out, arrived = lax.optimization_barrier((layer_out, arrived))
    outs = exchange(layer_out, GROUP)

    act_partial = jnp.einsum(
        "tc,rc->tr", arrived.reshape(zs * tokens, half_width), up_half, preferred_element_type=jnp.float32
    )
    act_other = swapped(act_partial.astype(jnp.bfloat16), "zh")
    shares = pl.pallas_call(
        share_body,
        in_specs=[SMEM] + [VMEM] * 5,
        out_specs=[VMEM] * xs,
        out_shape=[shape((zs * tokens, 2 * block + ranks))] * xs,
        name="share",
    )(place, inputs, arrived, act_partial, act_other, scale)
    shares = list(shares)
    for step in range(1, xs):
        shares[step] = shifted(shares[step], "x", step)

    everyone = sections * xs * zs
    products = pl.pallas_call(
        gram_body,
        in_specs=[VMEM] * 2,
        out_specs=VMEM,
        out_shape=shape((everyone, LANES), jnp.float32),
        name="gram",
    )(grads, outs)
    mixing = exchange(products, (*GROUP, "x", "zh")).sum(axis=0)[:MIXES]

    up_grad, down_grad, gain_grad = pl.pallas_call(
        weights_body,
        in_specs=[VMEM] * (2 * xs + 2),
        out_specs=[VMEM] * 3,
        out_shape=[shape((ranks, block)), shape((block, ranks)), shape((1, block), jnp.float32)],
        name="weights",
    )(*ups, *shares, norm_gain, down_proj[0])
    return (up_grad[None], down_grad[None], gain_grad, mixing[None])


def solution(mesh):
    devices = mesh.devices.reshape(4, 2, 8, 4, 2)
    fine = Mesh(devices, ("zl", "yh", "r", "x", "zh"))
    section, dp = (("zl", "yh", "r"), ("x", "zh"))
    return jax.shard_map(
        whole,
        mesh=fine,
        in_specs=(
            P(section, dp, None),
            P(section, dp, None),
            P(section, dp, None),
            P(section, dp, None),
            P(section, None, dp),
            P(section, dp),
            P(section, None),
        ),
        out_specs=(
            P(section, None, dp),
            P(section, dp, None),
            P(section, dp),
            P(section, None),
        ),
        check_vma=False,
    )
```

```python
import jax
import jax.numpy as jnp
from jax import lax
from jax.experimental import pallas as pl
from jax.experimental.pallas import tpu as pltpu
from jax.sharding import Mesh, PartitionSpec as P


MIXES = 8
LANES = 128
BLOCK = 640
TERMS = 3
epsilon = 1e-06
root_coef = 0.7978845608028654
GROUP = ("zl", "yh")
SMEM = pl.BlockSpec(memory_space=pltpu.SMEM)
VMEM = pl.BlockSpec(memory_space=pltpu.VMEM)


def gelu_pair(values):
    tangent = jnp.tanh(root_coef * (values + 0.044715 * values * values * values))
    result = 0.5 * values * (1.0 + tangent)
    slopes = 0.5 * (1.0 + tangent) + 0.5 * values * (1.0 - tangent * tangent) * root_coef * (
        1.0 + 3.0 * 0.044715 * values * values
    )
    return (result, slopes)


def exchange(pieces, axes):
    return lax.all_to_all(pieces, axes, split_axis=0, concat_axis=0, tiled=True)


def swapped(value, axis):
    return lax.ppermute(value, axis, [(0, 1), (1, 0)])


def shifted(value, axis, steps):
    count = lax.axis_size(axis)
    return lax.ppermute(value, axis, [(i, (i + steps) % count) for i in range(count)])


def split_terms(value):
    terms = []
    for _ in range(TERMS):
        term = value.astype(jnp.bfloat16).astype(jnp.float32)
        terms.append(term)
        value = value - term
    return terms


def shape(dims, dtype=jnp.bfloat16):
    return jax.ShapeDtypeStruct(dims, dtype)


def pack_grads_body(weights, grads, out):
    halves, sections, rows, cols = out.shape
    block = BLOCK
    for half in range(halves):
        for i in range((cols - LANES) // block):
            piece = grads[:, (i * halves + half) * block : (i * halves + half + 1) * block]
            out[half, :, :, i * block : (i + 1) * block] = piece.reshape(sections, rows, block)
    lane = lax.broadcasted_iota(jnp.int32, (rows, LANES), 1)
    row = lax.broadcasted_iota(jnp.int32, (rows, LANES), 0)
    value = jnp.zeros((rows, LANES), jnp.float32)
    for m in range(MIXES):
        value = jnp.where(lane == m, weights[0, m], value)
    tail = jnp.zeros((rows, LANES), jnp.float32)
    for i, term in enumerate(split_terms(value)):
        tail = jnp.where(row == i, term, tail)
    tail = tail.astype(jnp.bfloat16)
    for half in range(halves):
        for k in range(sections):
            out[half, k, :, cols - LANES :] = tail


def pack_inputs_body(place, layer_in, kept, sent):
    tokens, cols = kept.shape
    half_cols = cols - LANES
    width = layer_in.shape[1]
    block = BLOCK
    first = place[0] == 0
    squares = jnp.zeros((tokens, LANES), jnp.float32)
    for at in range(0, width, LANES):
        tile = layer_in[:, at : at + LANES].astype(jnp.float32)
        squares = squares + tile * tile
    inv_rms = lax.rsqrt(jnp.sum(squares, axis=1, keepdims=True) / width + epsilon)
    lane = lax.broadcasted_iota(jnp.int32, (tokens, LANES), 1)
    tail = jnp.zeros((tokens, LANES), jnp.float32)
    for i, term in enumerate(split_terms(jnp.broadcast_to(inv_rms, (tokens, LANES)))):
        tail = jnp.where(lane == i, term, tail)
    for i in range(half_cols // block):
        low = layer_in[:, 2 * i * block : (2 * i + 1) * block]
        high = layer_in[:, (2 * i + 1) * block : (2 * i + 2) * block]
        kept[:, i * block : (i + 1) * block] = jnp.where(first, low, high)
        sent[:, i * block : (i + 1) * block] = jnp.where(first, high, low)
    tail = tail.astype(jnp.bfloat16)
    kept[:, half_cols:] = tail
    sent[:, half_cols:] = tail


def activate_body(place, kept, other, up, act, slopes_out, out):
    sections, halves, rows, ranks = act.shape
    first = place[0] == 0
    for half in range(halves):
        near, far = (kept[...], other[...]) if half == 0 else (other[...], kept[...])
        values, slopes = gelu_pair(jnp.where(first, near, far).astype(jnp.float32))
        act[:, half] = values.astype(jnp.bfloat16)
        slopes_out[:, half] = slopes
    out[:, :BLOCK] = up[...]
    whole_act = act[...].reshape(sections * halves * rows, ranks).astype(jnp.float32)
    out[:, BLOCK:] = jnp.transpose(whole_act).astype(jnp.bfloat16)


def up_rows_body(place, up_0, up_1, up_2, up_3, out):
    for i in range(4):
        turn = lax.rem(place[1] - i + 4, 4)
        pieces = [up[:, :BLOCK] for up in (up_0, up_1, up_2, up_3)]
        near, far = (jnp.where(turn == 0, pieces[0], pieces[1]), jnp.where(turn == 2, pieces[2], pieces[3]))
        out[:, i * BLOCK : (i + 1) * BLOCK] = jnp.where(turn < 2, near, far)


def lift_body(place, kept, other, act, slopes, up_half, mixed, sends, scale, *moved):
    del mixed
    sections, halves, rows, width = sends.shape
    ranks = up_half.shape[0]
    first = place[0] == 0
    for half in range(halves):
        near, far = (kept, other) if half == 0 else (other, kept)
        terms = jnp.where(first, near[:, :, width:], far[:, :, width:]).astype(jnp.float32)
        scale[:, half] = slopes[:, half] * jnp.sum(terms, axis=2, keepdims=True)
        for step, out in enumerate(moved):
            at = pl.multiple_of(lax.rem(place[1] + step, len(moved)) * BLOCK, LANES)
            out[:, half] = jnp.where(first, near[:, :, pl.ds(at, BLOCK)], far[:, :, pl.ds(at, BLOCK)])
    for at in range(0, width, BLOCK):
        lanes = slice(at, at + BLOCK)
        for half in range(halves):
            near, far = (kept, other) if half == 0 else (other, kept)
            rows_in = jnp.where(first, near[:, :, lanes], far[:, :, lanes])
            branch = jnp.dot(
                act[:, half].reshape(sections * rows, ranks), up_half[:, lanes], preferred_element_type=jnp.float32
            ).reshape(sections, rows, BLOCK)
            sends[:, half, :, lanes] = (rows_in.astype(jnp.float32) + branch).astype(jnp.bfloat16)


def mix_body(coef, grads, out):
    sections, halves, _, cols = out.shape
    for half in range(halves):
        for at in range(0, cols, LANES):
            lanes = slice(at, at + LANES)
            tiles = [grads[half, k, :, lanes].astype(jnp.float32) for k in range(sections)]
            for k in range(sections):
                total = coef[k, 0] * tiles[k]
                for m in range(1, sections - k):
                    total = total + coef[k, m] * tiles[k + m]
                out[k, half, :, lanes] = total.astype(jnp.bfloat16)


def gram_body(grads, outs, result):
    sections, halves, rows, cols = outs.shape
    total = jnp.zeros((sections * rows, LANES), jnp.float32)
    for half in range(halves):
        total = total + lax.dot_general(
            outs[:, half].reshape(sections * rows, cols),
            grads[half, :, :, :cols].reshape(sections * rows, cols),
            (((1,), (1,)), ((), ())),
            preferred_element_type=jnp.float32,
        )
    row = lax.broadcasted_iota(jnp.int32, total.shape, 0)
    lane = lax.broadcasted_iota(jnp.int32, total.shape, 1)
    same = jnp.where(lax.rem(row, rows) == lax.rem(lane, rows), total, 0.0)
    share = result.shape[0] // sections
    spread = []
    for k in range(sections):
        sums = jnp.sum(same[k * rows : (k + 1) * rows], axis=0, keepdims=True)
        sums = jnp.broadcast_to(sums, (share, LANES))
        if k:
            sums = pltpu.roll(sums, LANES - k * rows, 1)
            sums = jnp.where(lane[:share] < LANES - k * rows, sums, 0.0)
        spread.append(sums)
    gather = jnp.where(lax.div(row, rows) == lane, 1.0, 0.0)
    result[...] = jnp.dot(
        jnp.concatenate(spread, axis=0), gather, precision=lax.Precision.HIGHEST, preferred_element_type=jnp.float32
    )


def share_body(place, grads, partial, other, scale, *outs):
    sections, halves, rows, _ = grads.shape
    count = sections * halves * rows
    latent_grad = ((partial[...] + other[...].astype(jnp.float32)) * scale[...]).astype(jnp.bfloat16)
    for step, out in enumerate(outs):
        at = pl.multiple_of(lax.rem(place[1] + step, len(outs)) * BLOCK, LANES)
        out[:, :BLOCK] = grads[:, :, :, pl.ds(at, BLOCK)].reshape(count, BLOCK)
        out[:, BLOCK:] = latent_grad


def weights_body(*refs):
    each = (len(refs) - 5) // 3
    acts, moved, shared = refs[:each], refs[each : 2 * each], refs[2 * each : 3 * each]
    gain, down, up_out, down_out, gain_out = refs[3 * each :]
    up_total = jnp.zeros(up_out.shape, jnp.float32)
    down_total = jnp.zeros(down_out.shape, jnp.float32)
    for act, inputs, piece in zip(acts, moved, shared):
        up_total = up_total + jnp.dot(act[:, BLOCK:], piece[:, :BLOCK], preferred_element_type=jnp.float32)
        down_total = down_total + lax.dot_general(
            inputs[...], piece[:, BLOCK:], (((0,), (0,)), ((), ())), preferred_element_type=jnp.float32
        )
    up_out[...] = up_total.astype(jnp.bfloat16)
    gain_cols = jnp.transpose(jnp.broadcast_to(gain[...].astype(jnp.float32), (8, gain.shape[1])))
    down_out[...] = (down_total * gain_cols[:, :1]).astype(jnp.bfloat16)
    product = down_total * down[...].astype(jnp.float32)
    ones = jnp.ones((8, product.shape[1]), jnp.float32)
    sums = lax.dot_general(
        ones, product, (((1,), (1,)), ((), ())), precision=lax.Precision.HIGHEST, preferred_element_type=jnp.float32
    )
    gain_out[...] = sums[:1]


def whole(layer_in, latent, mix_grad, down_proj, up_proj, norm_gain, mix_weight):
    layer_in, latent, mix_grad = (layer_in[0], latent[0], mix_grad[0])
    tokens, width = layer_in.shape
    ranks = latent.shape[1]
    xs, zs = (lax.axis_size("x"), lax.axis_size("zh"))
    sections = lax.axis_size("zl") * lax.axis_size("yh")
    block = width // (xs * zs)
    half_width = xs * block
    rows = tokens // sections
    place = jnp.stack([lax.axis_index("zh"), lax.axis_index("x")]).astype(jnp.int32)

    packed = pl.pallas_call(
        pack_grads_body,
        in_specs=[SMEM, pl.BlockSpec((tokens, width), lambda: (0, 0))],
        out_specs=pl.BlockSpec((zs, sections, rows, half_width + LANES), lambda: (0, 0, 0, 0)),
        out_shape=shape((zs, sections, rows, half_width + LANES)),
        name="pack_grads",
    )(mix_weight, mix_grad)
    grads = exchange(packed.reshape(zs * sections, rows, half_width + LANES), ("zh", *GROUP))
    grads = grads.reshape(zs, sections, rows, half_width + LANES)

    full = half_width + LANES
    kept, sent = pl.pallas_call(
        pack_inputs_body,
        in_specs=[SMEM, pl.BlockSpec((tokens, width), lambda: (0, 0))],
        out_specs=[pl.BlockSpec((tokens, full), lambda: (0, 0))] * 2,
        out_shape=[shape((tokens, full))] * 2,
        name="pack_inputs",
    )(place, layer_in)
    other = swapped(sent, "zh")
    other_latent = swapped(latent, "zh")
    kept, other, latent, other_latent = [
        t.reshape(sections, rows, t.shape[1]) for t in (kept, other, latent, other_latent)
    ]
    act, slopes, up_part = pl.pallas_call(
        activate_body,
        in_specs=[SMEM] + [VMEM] * 3,
        out_specs=[VMEM] * 3,
        out_shape=[
            shape((sections, zs, rows, ranks)),
            shape((sections, zs, rows, ranks), jnp.float32),
            shape((ranks, block + zs * tokens)),
        ],
        name="activate",
    )(place, latent, other_latent, up_proj[0])

    ups = [up_part]
    for step in range(1, xs):
        ups.append(shifted(up_part, "x", step))
    up_half = pl.pallas_call(
        up_rows_body,
        in_specs=[SMEM] + [VMEM] * xs,
        out_specs=VMEM,
        out_shape=shape((ranks, half_width)),
        name="up_rows",
    )(place, *ups)

    weights = jnp.sum(grads[0, :, :TERMS, half_width : half_width + MIXES].astype(jnp.float32), axis=1)
    chunk = shape((sections, zs, rows, half_width))
    mixed = pl.pallas_call(mix_body, in_specs=[SMEM, VMEM], out_specs=VMEM, out_shape=chunk, name="mix")(weights, grads)
    arrived = exchange(mixed, GROUP)

    layer_out, scale, *moved = pl.pallas_call(
        lift_body,
        in_specs=[SMEM] + [VMEM] * 5 + [pl.BlockSpec(memory_space=pl.ANY)],
        out_specs=[VMEM] * (2 + xs),
        out_shape=[chunk, shape((sections, zs, rows, ranks), jnp.float32)] + [shape((sections, zs, rows, block))] * xs,
        name="lift",
    )(place, kept, other, act, slopes, up_half, mixed)
    scale = scale.reshape(zs * tokens, ranks)
    for step in range(xs):
        moved[step] = moved[step].reshape(zs * tokens, block)
        if step:
            moved[step] = shifted(moved[step], "x", step)

    layer_out, arrived = lax.optimization_barrier((layer_out, arrived))
    outs = exchange(layer_out, GROUP)

    act_partial = jnp.einsum(
        "tc,rc->tr", arrived.reshape(zs * tokens, half_width), up_half, preferred_element_type=jnp.float32
    )
    act_other = swapped(act_partial.astype(jnp.bfloat16), "zh")
    shares = pl.pallas_call(
        share_body,
        in_specs=[SMEM] + [VMEM] * 4,
        out_specs=[VMEM] * xs,
        out_shape=[shape((zs * tokens, block + ranks))] * xs,
        name="share",
    )(place, arrived, act_partial, act_other, scale)
    shares = list(shares)
    for step in range(1, xs):
        shares[step] = shifted(shares[step], "x", step)

    everyone = sections * xs * zs
    products = pl.pallas_call(
        gram_body,
        in_specs=[VMEM] * 2,
        out_specs=VMEM,
        out_shape=shape((everyone, LANES), jnp.float32),
        name="gram",
    )(grads, outs)
    mixing = exchange(products, (*GROUP, "x", "zh")).sum(axis=0)[:MIXES]

    up_grad, down_grad, gain_grad = pl.pallas_call(
        weights_body,
        in_specs=[VMEM] * (3 * xs + 2),
        out_specs=[VMEM] * 3,
        out_shape=[shape((ranks, block)), shape((block, ranks)), shape((1, block), jnp.float32)],
        name="weights",
    )(*ups, *moved, *shares, norm_gain, down_proj[0])
    return (up_grad[None], down_grad[None], gain_grad, mixing[None])


def solution(mesh):
    devices = mesh.devices.reshape(4, 2, 8, 4, 2)
    fine = Mesh(devices, ("zl", "yh", "r", "x", "zh"))
    section, dp = (("zl", "yh", "r"), ("x", "zh"))
    return jax.shard_map(
        whole,
        mesh=fine,
        in_specs=(
            P(section, dp, None),
            P(section, dp, None),
            P(section, dp, None),
            P(section, dp, None),
            P(section, None, dp),
            P(section, dp),
            P(section, None),
        ),
        out_specs=(
            P(section, None, dp),
            P(section, dp, None),
            P(section, dp),
            P(section, None),
        ),
        check_vma=False,
    )
```

```python
import jax
import jax.numpy as jnp
from jax import lax
from jax.experimental import pallas as pl
from jax.experimental.pallas import tpu as pltpu
from jax.sharding import Mesh, PartitionSpec as P


MIXES = 8
LANES = 128
BLOCK = 640
TERMS = 3
epsilon = 1e-06
root_coef = 0.7978845608028654
GROUP = ("zl", "yh")
SMEM = pl.BlockSpec(memory_space=pltpu.SMEM)
VMEM = pl.BlockSpec(memory_space=pltpu.VMEM)


def gelu_pair(values):
    tangent = jnp.tanh(root_coef * (values + 0.044715 * values * values * values))
    result = 0.5 * values * (1.0 + tangent)
    slopes = 0.5 * (1.0 + tangent) + 0.5 * values * (1.0 - tangent * tangent) * root_coef * (
        1.0 + 3.0 * 0.044715 * values * values
    )
    return (result, slopes)


def exchange(pieces, axes):
    return lax.all_to_all(pieces, axes, split_axis=0, concat_axis=0, tiled=True)


def swapped(value, axis):
    return lax.ppermute(value, axis, [(0, 1), (1, 0)])


def shifted(value, axis, steps):
    count = lax.axis_size(axis)
    return lax.ppermute(value, axis, [(i, (i + steps) % count) for i in range(count)])


def split_terms(value):
    terms = []
    for _ in range(TERMS):
        term = value.astype(jnp.bfloat16).astype(jnp.float32)
        terms.append(term)
        value = value - term
    return terms


def shape(dims, dtype=jnp.bfloat16):
    return jax.ShapeDtypeStruct(dims, dtype)


def pack_grads_body(weights, grads, out):
    halves, sections, rows, cols = out.shape
    block = BLOCK
    for half in range(halves):
        for i in range((cols - LANES) // block):
            piece = grads[:, (i * halves + half) * block : (i * halves + half + 1) * block]
            out[half, :, :, i * block : (i + 1) * block] = piece.reshape(sections, rows, block)
    lane = lax.broadcasted_iota(jnp.int32, (rows, LANES), 1)
    row = lax.broadcasted_iota(jnp.int32, (rows, LANES), 0)
    value = jnp.zeros((rows, LANES), jnp.float32)
    for m in range(MIXES):
        value = jnp.where(lane == m, weights[0, m], value)
    tail = jnp.zeros((rows, LANES), jnp.float32)
    for i, term in enumerate(split_terms(value)):
        tail = jnp.where(row == i, term, tail)
    tail = tail.astype(jnp.bfloat16)
    for half in range(halves):
        for k in range(sections):
            out[half, k, :, cols - LANES :] = tail


def pack_inputs_body(place, layer_in, kept, sent):
    tokens, cols = kept.shape
    half_cols = cols - LANES
    width = layer_in.shape[1]
    block = BLOCK
    first = place[0] == 0
    squares = jnp.zeros((tokens, LANES), jnp.float32)
    for at in range(0, width, LANES):
        tile = layer_in[:, at : at + LANES].astype(jnp.float32)
        squares = squares + tile * tile
    inv_rms = lax.rsqrt(jnp.sum(squares, axis=1, keepdims=True) / width + epsilon)
    lane = lax.broadcasted_iota(jnp.int32, (tokens, LANES), 1)
    tail = jnp.zeros((tokens, LANES), jnp.float32)
    for i, term in enumerate(split_terms(jnp.broadcast_to(inv_rms, (tokens, LANES)))):
        tail = jnp.where(lane == i, term, tail)
    for i in range(half_cols // block):
        low = layer_in[:, 2 * i * block : (2 * i + 1) * block]
        high = layer_in[:, (2 * i + 1) * block : (2 * i + 2) * block]
        kept[:, i * block : (i + 1) * block] = jnp.where(first, low, high)
        sent[:, i * block : (i + 1) * block] = jnp.where(first, high, low)
    tail = tail.astype(jnp.bfloat16)
    kept[:, half_cols:] = tail
    sent[:, half_cols:] = tail


def activate_body(place, kept, other, up, act, slopes_out, out):
    sections, halves, rows, ranks = act.shape
    first = place[0] == 0
    for half in range(halves):
        near, far = (kept[...], other[...]) if half == 0 else (other[...], kept[...])
        values, slopes = gelu_pair(jnp.where(first, near, far).astype(jnp.float32))
        act[:, half] = values.astype(jnp.bfloat16)
        slopes_out[:, half] = slopes
    out[:, :BLOCK] = up[...]
    whole_act = act[...].reshape(sections * halves * rows, ranks).astype(jnp.float32)
    out[:, BLOCK:] = jnp.transpose(whole_act).astype(jnp.bfloat16)


def up_rows_body(place, up_0, up_1, up_2, up_3, mixed, out):
    del mixed
    for i in range(4):
        turn = lax.rem(place[1] - i + 4, 4)
        pieces = [up[:, :BLOCK] for up in (up_0, up_1, up_2, up_3)]
        near, far = (jnp.where(turn == 0, pieces[0], pieces[1]), jnp.where(turn == 2, pieces[2], pieces[3]))
        out[:, i * BLOCK : (i + 1) * BLOCK] = jnp.where(turn < 2, near, far)


def lift_body(place, kept, other, act, slopes, up_half, mixed, sends, scale, *moved):
    del mixed
    sections, halves, rows, width = sends.shape
    ranks = up_half.shape[0]
    first = place[0] == 0
    for half in range(halves):
        near, far = (kept, other) if half == 0 else (other, kept)
        terms = jnp.where(first, near[:, :, width:], far[:, :, width:]).astype(jnp.float32)
        scale[:, half] = slopes[:, half] * jnp.sum(terms, axis=2, keepdims=True)
        for step, out in enumerate(moved):
            at = pl.multiple_of(lax.rem(place[1] + step, len(moved)) * BLOCK, LANES)
            out[:, half] = jnp.where(first, near[:, :, pl.ds(at, BLOCK)], far[:, :, pl.ds(at, BLOCK)])
    for at in range(0, width, BLOCK):
        lanes = slice(at, at + BLOCK)
        for half in range(halves):
            near, far = (kept, other) if half == 0 else (other, kept)
            rows_in = jnp.where(first, near[:, :, lanes], far[:, :, lanes])
            branch = jnp.dot(
                act[:, half].reshape(sections * rows, ranks), up_half[:, lanes], preferred_element_type=jnp.float32
            ).reshape(sections, rows, BLOCK)
            sends[:, half, :, lanes] = (rows_in.astype(jnp.float32) + branch).astype(jnp.bfloat16)


def mix_body(place, coef, grads, *refs):
    outs, out = refs[:-1], refs[-1]
    sections, halves, _, cols = out.shape
    for half in range(halves):
        for at in range(0, cols, LANES):
            lanes = slice(at, at + LANES)
            tiles = [grads[half, k, :, lanes].astype(jnp.float32) for k in range(sections)]
            for k in range(sections):
                total = coef[k, 0] * tiles[k]
                for m in range(1, sections - k):
                    total = total + coef[k, m] * tiles[k + m]
                out[k, half, :, lanes] = total.astype(jnp.bfloat16)
    for step, ref in enumerate(outs):
        ref[...] = out[lax.bitwise_xor(place[2], step)]


def order_body(place, *refs):
    pieces, out = refs[:-1], refs[-1]
    for step, piece in enumerate(pieces):
        out[lax.bitwise_xor(place[2], step)] = piece[...]


def gram_body(grads, outs, result):
    sections, halves, rows, cols = outs.shape
    total = jnp.zeros((sections * rows, LANES), jnp.float32)
    for half in range(halves):
        total = total + lax.dot_general(
            outs[:, half].reshape(sections * rows, cols),
            grads[half, :, :, :cols].reshape(sections * rows, cols),
            (((1,), (1,)), ((), ())),
            preferred_element_type=jnp.float32,
        )
    row = lax.broadcasted_iota(jnp.int32, total.shape, 0)
    lane = lax.broadcasted_iota(jnp.int32, total.shape, 1)
    same = jnp.where(lax.rem(row, rows) == lax.rem(lane, rows), total, 0.0)
    share = result.shape[0] // sections
    spread = []
    for k in range(sections):
        sums = jnp.sum(same[k * rows : (k + 1) * rows], axis=0, keepdims=True)
        sums = jnp.broadcast_to(sums, (share, LANES))
        if k:
            sums = pltpu.roll(sums, LANES - k * rows, 1)
            sums = jnp.where(lane[:share] < LANES - k * rows, sums, 0.0)
        spread.append(sums)
    gather = jnp.where(lax.div(row, rows) == lane, 1.0, 0.0)
    result[...] = jnp.dot(
        jnp.concatenate(spread, axis=0), gather, precision=lax.Precision.HIGHEST, preferred_element_type=jnp.float32
    )


def share_body(place, grads, partial, other, scale, *outs):
    sections, halves, rows, _ = grads.shape
    count = sections * halves * rows
    latent_grad = ((partial[...] + other[...].astype(jnp.float32)) * scale[...]).astype(jnp.bfloat16)
    for step, out in enumerate(outs):
        at = pl.multiple_of(lax.rem(place[1] + step, len(outs)) * BLOCK, LANES)
        out[:, :BLOCK] = grads[:, :, :, pl.ds(at, BLOCK)].reshape(count, BLOCK)
        out[:, BLOCK:] = latent_grad


def weights_body(*refs):
    each = (len(refs) - 5) // 3
    acts, moved, shared = refs[:each], refs[each : 2 * each], refs[2 * each : 3 * each]
    gain, down, up_out, down_out, gain_out = refs[3 * each :]
    up_total = jnp.zeros(up_out.shape, jnp.float32)
    down_total = jnp.zeros(down_out.shape, jnp.float32)
    for act, inputs, piece in zip(acts, moved, shared):
        up_total = up_total + jnp.dot(act[:, BLOCK:], piece[:, :BLOCK], preferred_element_type=jnp.float32)
        down_total = down_total + lax.dot_general(
            inputs[...], piece[:, BLOCK:], (((0,), (0,)), ((), ())), preferred_element_type=jnp.float32
        )
    up_out[...] = up_total.astype(jnp.bfloat16)
    gain_cols = jnp.transpose(jnp.broadcast_to(gain[...].astype(jnp.float32), (8, gain.shape[1])))
    down_out[...] = (down_total * gain_cols[:, :1]).astype(jnp.bfloat16)
    product = down_total * down[...].astype(jnp.float32)
    ones = jnp.ones((8, product.shape[1]), jnp.float32)
    sums = lax.dot_general(
        ones, product, (((1,), (1,)), ((), ())), precision=lax.Precision.HIGHEST, preferred_element_type=jnp.float32
    )
    gain_out[...] = sums[:1]


def whole(layer_in, latent, mix_grad, down_proj, up_proj, norm_gain, mix_weight):
    layer_in, latent, mix_grad = (layer_in[0], latent[0], mix_grad[0])
    tokens, width = layer_in.shape
    ranks = latent.shape[1]
    xs, zs = (lax.axis_size("x"), lax.axis_size("zh"))
    sections = lax.axis_size("zl") * lax.axis_size("yh")
    block = width // (xs * zs)
    half_width = xs * block
    rows = tokens // sections
    at_group = lax.axis_index("zl") * lax.axis_size("yh") + lax.axis_index("yh")
    place = jnp.stack([lax.axis_index("zh"), lax.axis_index("x"), at_group]).astype(jnp.int32)

    packed = pl.pallas_call(
        pack_grads_body,
        in_specs=[SMEM, pl.BlockSpec((tokens, width), lambda: (0, 0))],
        out_specs=pl.BlockSpec((zs, sections, rows, half_width + LANES), lambda: (0, 0, 0, 0)),
        out_shape=shape((zs, sections, rows, half_width + LANES)),
        name="pack_grads",
    )(mix_weight, mix_grad)
    grads = exchange(packed.reshape(zs * sections, rows, half_width + LANES), ("zh", *GROUP))
    grads = grads.reshape(zs, sections, rows, half_width + LANES)

    full = half_width + LANES
    kept, sent = pl.pallas_call(
        pack_inputs_body,
        in_specs=[SMEM, pl.BlockSpec((tokens, width), lambda: (0, 0))],
        out_specs=[pl.BlockSpec((tokens, full), lambda: (0, 0))] * 2,
        out_shape=[shape((tokens, full))] * 2,
        name="pack_inputs",
    )(place, layer_in)
    other = swapped(sent, "zh")
    other_latent = swapped(latent, "zh")
    kept, other, latent, other_latent = [
        t.reshape(sections, rows, t.shape[1]) for t in (kept, other, latent, other_latent)
    ]
    act, slopes, up_part = pl.pallas_call(
        activate_body,
        in_specs=[SMEM] + [VMEM] * 3,
        out_specs=[VMEM] * 3,
        out_shape=[
            shape((sections, zs, rows, ranks)),
            shape((sections, zs, rows, ranks), jnp.float32),
            shape((ranks, block + zs * tokens)),
        ],
        name="activate",
    )(place, latent, other_latent, up_proj[0])

    ups = [up_part]
    for step in range(1, xs):
        ups.append(shifted(up_part, "x", step))
    weights = jnp.sum(grads[0, :, :TERMS, half_width : half_width + MIXES].astype(jnp.float32), axis=1)
    chunk = shape((sections, zs, rows, half_width))
    mixed = pl.pallas_call(
        mix_body,
        in_specs=[SMEM, SMEM, VMEM],
        out_specs=[VMEM] * sections,
        out_shape=[shape(chunk.shape[1:])] * sections,
        scratch_shapes=[pltpu.VMEM(chunk.shape, jnp.bfloat16)],
        name="mix",
    )(place, weights, grads)
    arrived = [mixed[0]]
    for step in range(1, sections):
        arrived.append(lax.ppermute(mixed[step], GROUP, [(k, k ^ step) for k in range(sections)]))
    arrived = pl.pallas_call(
        order_body, in_specs=[SMEM] + [VMEM] * sections, out_specs=VMEM, out_shape=chunk, name="order"
    )(place, *arrived)

    up_half = pl.pallas_call(
        up_rows_body,
        in_specs=[SMEM] + [VMEM] * xs + [pl.BlockSpec(memory_space=pl.ANY)],
        out_specs=VMEM,
        out_shape=shape((ranks, half_width)),
        name="up_rows",
    )(place, *ups, mixed[0])
    layer_out, scale, *moved = pl.pallas_call(
        lift_body,
        in_specs=[SMEM] + [VMEM] * 5 + [pl.BlockSpec(memory_space=pl.ANY)],
        out_specs=[VMEM] * (2 + xs),
        out_shape=[chunk, shape((sections, zs, rows, ranks), jnp.float32)] + [shape((sections, zs, rows, block))] * xs,
        name="lift",
    )(place, kept, other, act, slopes, up_half, mixed[0])
    scale = scale.reshape(zs * tokens, ranks)
    for step in range(xs):
        moved[step] = moved[step].reshape(zs * tokens, block)
        if step:
            moved[step] = shifted(moved[step], "x", step)

    outs = exchange(layer_out, GROUP)

    act_partial = jnp.einsum(
        "tc,rc->tr", arrived.reshape(zs * tokens, half_width), up_half, preferred_element_type=jnp.float32
    )
    act_other = swapped(act_partial.astype(jnp.bfloat16), "zh")
    shares = pl.pallas_call(
        share_body,
        in_specs=[SMEM] + [VMEM] * 4,
        out_specs=[VMEM] * xs,
        out_shape=[shape((zs * tokens, block + ranks))] * xs,
        name="share",
    )(place, arrived, act_partial, act_other, scale)
    shares = list(shares)
    for step in range(1, xs):
        shares[step] = shifted(shares[step], "x", step)

    everyone = sections * xs * zs
    products = pl.pallas_call(
        gram_body,
        in_specs=[VMEM] * 2,
        out_specs=VMEM,
        out_shape=shape((everyone, LANES), jnp.float32),
        name="gram",
    )(grads, outs)
    mixing = exchange(products, (*GROUP, "x", "zh")).sum(axis=0)[:MIXES]

    up_grad, down_grad, gain_grad = pl.pallas_call(
        weights_body,
        in_specs=[VMEM] * (3 * xs + 2),
        out_specs=[VMEM] * 3,
        out_shape=[shape((ranks, block)), shape((block, ranks)), shape((1, block), jnp.float32)],
        name="weights",
    )(*ups, *moved, *shares, norm_gain, down_proj[0])
    return (up_grad[None], down_grad[None], gain_grad, mixing[None])


def solution(mesh):
    devices = mesh.devices.reshape(4, 2, 8, 4, 2)
    fine = Mesh(devices, ("zl", "yh", "r", "x", "zh"))
    section, dp = (("zl", "yh", "r"), ("x", "zh"))
    return jax.shard_map(
        whole,
        mesh=fine,
        in_specs=(
            P(section, dp, None),
            P(section, dp, None),
            P(section, dp, None),
            P(section, dp, None),
            P(section, None, dp),
            P(section, dp),
            P(section, None),
        ),
        out_specs=(
            P(section, None, dp),
            P(section, dp, None),
            P(section, dp),
            P(section, None),
        ),
        check_vma=False,
    )
```
